8 devices in a mesh: dp: 2 (over z, y), fsdp: 4 (over x, core).
Axes of the slice: x: 2, y: 2, z: 1, core: 2. Of those that a mesh axis runs over, the one named last changes fastest.
Arguments:
- x_in: bfloat16 [128, 256, 512], P(('dp', 'fsdp'))
- grad_y: bfloat16 [128, 256, 512], P(('dp', 'fsdp'))
- norm_scale: bfloat16 [2, 512], P(None, 'fsdp')
- w_in: bfloat16 [2, 512, 4736], P(None, 'fsdp')
- w_out: bfloat16 [2, 2560, 512], P(None, 'fsdp')
Outputs:
- output 1: bfloat16 [128, 256, 512], P(('dp', 'fsdp'))
- output 2: bfloat16 [128, 256, 512], P(('dp', 'fsdp'))
- output 3: float32 [2, 512], P(None, 'fsdp')
- output 4: float32 [2, 512, 4736], P(None, 'fsdp')
- output 5: float32 [2, 2560, 512], P(None, 'fsdp')
All inputs are finite; a program needn't handle non-finite values.
Results may differ from the reference program's by a relative error of at most 0.0145983.
Values are sent between devices in bfloat16 or wider.
A program may use at most 1 GiB of HBM per device.

```python
import jax
import jax.numpy as jnp
from jax import lax

MODEL_DIM = 512
N_HEADS = 8
HEAD_DIM = 64
FF_DIM = 2048
SEQ_LEN = 256
BATCH = 128
N_LAYERS = 2

PROJ_DIM = MODEL_DIM + 2 * HEAD_DIM + 2 * FF_DIM
CAT_DIM = MODEL_DIM + FF_DIM


def setup_inputs(seed: int = 0) -> dict:
    rng_keys = jax.random.split(jax.random.key(seed), 5)
    x_in = jax.random.normal(rng_keys[0], (BATCH, SEQ_LEN, MODEL_DIM), jnp.float32)
    grad_y = jax.random.normal(rng_keys[1], (BATCH, SEQ_LEN, MODEL_DIM), jnp.float32)
    norm_scale = 1.0 + 0.3 * jax.random.normal(rng_keys[2], (N_LAYERS, MODEL_DIM), jnp.float32)
    w_in = jax.random.normal(rng_keys[3], (N_LAYERS, MODEL_DIM, PROJ_DIM), jnp.float32) * MODEL_DIM ** -0.5
    w_out = jax.random.normal(rng_keys[4], (N_LAYERS, CAT_DIM, MODEL_DIM), jnp.float32) * CAT_DIM ** -0.5
    return {
        "x_in": x_in.astype(jnp.bfloat16),
        "grad_y": grad_y.astype(jnp.bfloat16),
        "norm_scale": norm_scale.astype(jnp.bfloat16),
        "w_in": w_in.astype(jnp.bfloat16),
        "w_out": w_out.astype(jnp.bfloat16),
    }


def layer_norm(hidden, gain_vec):
    hid_f32 = hidden.astype(jnp.float32)
    centered = hid_f32 - jnp.mean(hid_f32, axis=-1, keepdims=True)
    variance = jnp.mean(centered * centered, axis=-1, keepdims=True)
    return (centered * lax.rsqrt(variance + 1e-6) * gain_vec).astype(jnp.bfloat16)


def rotary_tables():
    half_dim = HEAD_DIM // 2
    inv_freq = 10000.0 ** (-(jnp.arange(half_dim, dtype=jnp.float32) * 2.0 / HEAD_DIM))
    angles = jnp.arange(SEQ_LEN, dtype=jnp.float32)[:, None] * inv_freq[None, :]
    return jnp.cos(angles), jnp.sin(angles)


def rotate(vectors, cos_tab, sin_tab):
    half_dim = vectors.shape[-1] // 2
    lo_half = vectors[..., :half_dim]
    hi_half = vectors[..., half_dim:]
    return jnp.concatenate([lo_half * cos_tab - hi_half * sin_tab, hi_half * cos_tab + lo_half * sin_tab], axis=-1)


def mix_seq(projected):
    kv_end = MODEL_DIM + 2 * HEAD_DIM
    queries = projected[:, :MODEL_DIM].reshape(SEQ_LEN, N_HEADS, HEAD_DIM).astype(jnp.float32) * HEAD_DIM ** -0.5
    key_vec = projected[:, MODEL_DIM:MODEL_DIM + HEAD_DIM].astype(jnp.float32)
    val_vec = projected[:, MODEL_DIM + HEAD_DIM:kv_end].astype(jnp.float32)
    gate_act = projected[:, kv_end:kv_end + FF_DIM].astype(jnp.float32)
    up_act = projected[:, kv_end + FF_DIM:].astype(jnp.float32)
    cos_tab, sin_tab = rotary_tables()
    q_rot = rotate(queries, cos_tab[:, None, :], sin_tab[:, None, :]).astype(jnp.bfloat16).astype(jnp.float32)
    k_rot = rotate(key_vec, cos_tab, sin_tab).astype(jnp.bfloat16).astype(jnp.float32)
    scores = jnp.einsum("qhd,kd->hqk", q_rot, k_rot)
    positions = jnp.arange(SEQ_LEN)
    scores = jnp.where(positions[:, None] >= positions[None, :], scores, -1e30)
    attn_probs = jax.nn.softmax(scores, axis=-1).astype(jnp.bfloat16).astype(jnp.float32)
    attn_out = jnp.einsum("hqk,kd->qhd", attn_probs, val_vec).astype(jnp.bfloat16).reshape(SEQ_LEN, MODEL_DIM)
    mlp_out = (jax.nn.silu(gate_act) * up_act).astype(jnp.bfloat16)
    return jnp.concatenate([attn_out, mlp_out], axis=-1)


def mix_backward(seq_pair):
    projected, grad_mixed = seq_pair
    return jax.vjp(mix_seq, projected)[1](grad_mixed)[0]


def layer_forward(hidden, gain_vec, w_in_l, w_out_l):
    normed = layer_norm(hidden, gain_vec.astype(jnp.float32))
    projected = jnp.dot(normed.reshape(-1, MODEL_DIM), w_in_l, preferred_element_type=jnp.float32).astype(jnp.bfloat16)
    projected = projected.reshape(BATCH, SEQ_LEN, PROJ_DIM)
    mixed_out = lax.map(mix_seq, projected)
    block_out = jnp.dot(mixed_out.reshape(-1, CAT_DIM), w_out_l, preferred_element_type=jnp.float32)
    layer_out = (hidden.astype(jnp.float32) + block_out.reshape(BATCH, SEQ_LEN, MODEL_DIM)).astype(jnp.bfloat16)
    return layer_out, normed, projected, mixed_out


def layer_backward(hidden, gain_vec, w_in_l, w_out_l, grad_out):
    normed, projected, mixed_out = layer_forward(hidden, gain_vec, w_in_l, w_out_l)[1:]
    grad_rows = grad_out.reshape(-1, MODEL_DIM)
    grad_w_out = jnp.dot(mixed_out.reshape(-1, CAT_DIM).T, grad_rows, preferred_element_type=jnp.float32)
    grad_mixed = jnp.dot(grad_rows, w_out_l.T, preferred_element_type=jnp.float32).astype(jnp.bfloat16)
    grad_proj = lax.map(mix_backward, (projected, grad_mixed.reshape(BATCH, SEQ_LEN, CAT_DIM)))
    grad_proj_rows = grad_proj.reshape(-1, PROJ_DIM)
    grad_w_in = jnp.dot(normed.reshape(-1, MODEL_DIM).T, grad_proj_rows, preferred_element_type=jnp.float32)
    grad_normed = jnp.dot(grad_proj_rows, w_in_l.T, preferred_element_type=jnp.float32).astype(jnp.bfloat16)
    norm_vjp = jax.vjp(layer_norm, hidden, gain_vec.astype(jnp.float32))[1]
    grad_hidden, grad_gain = norm_vjp(grad_normed.reshape(BATCH, SEQ_LEN, MODEL_DIM))
    grad_in = (grad_out.astype(jnp.float32) + grad_hidden.astype(jnp.float32)).astype(jnp.bfloat16)
    return grad_in, grad_gain, grad_w_in, grad_w_out


def reference(x_in, grad_y, norm_scale, w_in, w_out):
    layer_inputs = []
    hidden = x_in
    for layer_idx in range(N_LAYERS):
        layer_inputs.append(hidden)
        hidden = layer_forward(hidden, norm_scale[layer_idx], w_in[layer_idx], w_out[layer_idx])[0]
    grad_hidden = grad_y
    scale_grads = []
    in_grads = []
    out_grads = []
    for layer_idx in reversed(range(N_LAYERS)):
        grad_hidden, grad_gain, grad_w_in, grad_w_out = layer_backward(
            layer_inputs[layer_idx], norm_scale[layer_idx], w_in[layer_idx], w_out[layer_idx], grad_hidden)
        scale_grads.append(grad_gain)
        in_grads.append(grad_w_in)
        out_grads.append(grad_w_out)
    return (hidden, grad_hidden, jnp.stack(scale_grads[::-1]), jnp.stack(in_grads[::-1]), jnp.stack(out_grads[::-1]))
```

```python
import functools
import jax
import jax.numpy as jnp
from jax import lax
from jax.experimental import pallas as pl
from jax.experimental.pallas import tpu as pltpu
from jax.sharding import PartitionSpec as P

F32 = jnp.float32
BF16 = jnp.bfloat16
SEQ = 256
HD = 64
D = 512
FF = 2048
QKV = D + 2 * HD
NEG = -1e30
VMEM_LIMIT = 60 * 1024 * 1024

TOK = 512


def dot(a, b):
    return jnp.dot(a, b, preferred_element_type=F32)


def dot_nt(a, b):
    return lax.dot_general(a, b, (((1,), (1,)), ((), ())), preferred_element_type=F32)


def dot_tn(a, b):
    return lax.dot_general(a, b, (((0,), (0,)), ((), ())), preferred_element_type=F32)


def owners():
    me = lax.axis_index("fsdp")
    x = me // 2
    c = me - 2 * x
    return [2 * x + c, 2 * x + (1 - c), 2 * (1 - x) + c, 2 * (1 - x) + (1 - c)]


def load_rows(groups, sem):
    own = owners()
    copies = []
    for pieces, dst in groups:
        rows = pieces[0].shape[0]
        for r in range(4):
            start = pl.multiple_of(own[r] * rows, rows)
            src = pieces[r].at[:, pl.ds(0, dst.shape[1])]
            cp = pltpu.make_async_copy(src, dst.at[pl.ds(start, rows), :], sem.at[len(copies)])
            cp.start()
            copies.append(cp)
    for cp in copies:
        cp.wait()


def lane_iota(shape):
    return lax.broadcasted_iota(jnp.int32, shape, len(shape) - 1)


def half_swap(z):
    n = z.shape[-1]
    lo = lax.rem(lane_iota(z.shape), HD) < HD // 2
    return jnp.where(lo, pltpu.roll(z, n - HD // 2, 1), pltpu.roll(z, HD // 2, 1))


HALF = SEQ // 2


def kv_tiles(kv):
    lo = lane_iota(kv.shape) < HD
    rolled = pltpu.roll(kv, HD, 1)
    zero = jnp.zeros_like(kv)
    return (jnp.where(lo, kv, zero), jnp.where(lo, zero, rolled),
            jnp.where(lo, rolled, zero), jnp.where(lo, zero, kv))


def tri_mask(n):
    key = lax.broadcasted_iota(jnp.int32, (HALF, n), 0)
    query = lax.rem(lax.broadcasted_iota(jnp.int32, (HALF, n), 1), HALF)
    return query >= key


def softmax_keys(s, n_keys, tri):
    out = []
    for i in range(2):
        sh = s[i * n_keys:(i + 1) * n_keys]
        sh = [sh[k * HALF:(k + 1) * HALF] for k in range(n_keys // HALF)]
        sh[-1] = jnp.where(tri, sh[-1], NEG)
        m = jnp.max(sh[-1], axis=0, keepdims=True)
        for t in sh[:-1]:
            m = jnp.maximum(m, jnp.max(t, axis=0, keepdims=True))
        e = [jnp.exp(t - m) for t in sh]
        l = jnp.sum(e[0], axis=0, keepdims=True)
        for t in e[1:]:
            l = l + jnp.sum(t, axis=0, keepdims=True)
        inv = 1.0 / l
        out.append([t * inv for t in e])
    return out


def fwd_attn_kernel(x_ref, gain_ref, c_ref, s_ref, w0, w1, w2, w3, h_ref, qkv_ref, o_ref, w_ref, sem):
    @pl.when(pl.program_id(0) == 0)
    def _():
        load_rows([((w0, w1, w2, w3), w_ref)], sem)

    x = x_ref[...].astype(F32)
    cen = x - jnp.mean(x, axis=-1, keepdims=True)
    var = jnp.mean(cen * cen, axis=-1, keepdims=True)
    h = (cen * lax.rsqrt(var + 1e-6) * gain_ref[...]).astype(BF16)
    h_ref[...] = h
    z_all = dot(h, w_ref[...]).astype(BF16)
    tri = tri_mask(128)
    for b in range(TOK // SEQ):
        r0 = b * SEQ
        zt = []
        for j in range(5):
            t = z_all[r0:r0 + SEQ, j * 128:(j + 1) * 128].astype(F32)
            tc = slice(0, 128) if j < 4 else slice(128, 256)
            t = (t * c_ref[:, tc] + half_swap(t) * s_ref[:, tc]).astype(BF16)
            qkv_ref[r0:r0 + SEQ, j * 128:(j + 1) * 128] = t
            zt.append(t)
        k0, k1, v0, v1 = kv_tiles(zt[4].astype(F32))
        k0, k1 = k0.astype(BF16), k1.astype(BF16)
        v0, v1 = v0.T.astype(BF16), v1.T.astype(BF16)
        for blk in range(2):
            nk = (blk + 1) * HALF
            rows = slice(blk * HALF, (blk + 1) * HALF)
            k_st = jnp.concatenate([k0[:nk], k1[:nk]], axis=0)
            v_t = jnp.concatenate([v0[:, :nk], v1[:, :nk]], axis=1)
            for g in range(2):
                q = jnp.concatenate([zt[2 * g + i][rows] for i in range(2)], axis=0)
                s = dot_nt(k_st, q)
                trib = jnp.concatenate([tri] * 2, axis=1)
                p = softmax_keys(s, nk, trib)
                pb = jnp.concatenate([t.astype(BF16) for ph in p for t in ph], axis=0)
                o = dot(v_t, pb).T.astype(BF16)
                for i in range(2):
                    j = 2 * g + i
                    o_ref[r0 + blk * HALF:r0 + (blk + 1) * HALF, j * 128:(j + 1) * 128] = o[i * HALF:(i + 1) * HALF]


def fwd_mlp_kernel(x_ref, h_ref, o_ref, g0, g1, g2, g3, u0, u1, u2, u3, z_ref, m_ref, y_ref, w_ref, wo_ref, sem):
    @pl.when(pl.program_id(0) == 0)
    def _():
        load_rows([((g0, g1, g2, g3), w_ref), ((u0, u1, u2, u3), wo_ref)], sem)

    h = h_ref[...]
    cw = 512
    acc = dot(o_ref[...], wo_ref[0:D, :])
    for c in range(FF // cw):
        gc = slice(c * cw, (c + 1) * cw)
        uc = slice(FF + c * cw, FF + (c + 1) * cw)
        g = dot(h, w_ref[:, gc]).astype(BF16)
        u = dot(h, w_ref[:, uc]).astype(BF16)
        z_ref[:, gc] = g
        z_ref[:, uc] = u
        g = g.astype(F32)
        m = (g * jax.nn.sigmoid(g) * u.astype(F32)).astype(BF16)
        m_ref[:, gc] = m
        acc = acc + dot(m, wo_ref[D + c * cw:D + (c + 1) * cw, :])
    y_ref[...] = (x_ref[...].astype(F32) + acc).astype(BF16)


def store_grad_rows(acc, width, own_ref, xp_ref, send_ref, sem, by_cols):
    move_grad_rows(acc, width, own_ref, xp_ref, send_ref, sem, by_cols, False)


def move_grad_rows(acc, width, own_ref, xp_ref, send_ref, sem, by_cols, inward):
    own = owners()
    copies = []
    for r, dst in enumerate((own_ref, send_ref.at[0], xp_ref, send_ref.at[1])):
        start = pl.multiple_of(own[r] * width, 128)
        src = acc.at[:, pl.ds(start, width)] if by_cols else acc.at[pl.ds(start, width), :]
        if inward:
            src, dst = dst, src
        cp = pltpu.make_async_copy(src, dst, sem.at[r])
        cp.start()
        copies.append(cp)
    for cp in copies:
        cp.wait()


def dwo_kernel(dy_ref, o_ref, m_ref, own_ref, xp_ref, send_ref, acc, sem):
    step = pl.program_id(0)

    @pl.when(step == 0)
    def _():
        acc[...] = jnp.zeros_like(acc)

    dy = dy_ref[...]
    acc[:, 0:D] += dot_tn(dy, o_ref[...])
    cw = 512
    for c in range(FF // cw):
        acc[:, D + c * cw:D + (c + 1) * cw] += dot_tn(dy, m_ref[:, c * cw:(c + 1) * cw])

    @pl.when(step == pl.num_programs(0) - 1)
    def _():
        store_grad_rows(acc, (D + FF) // 4, own_ref, xp_ref, send_ref, sem, True)


def bmlp_kernel(half, dy_ref, h_ref, zg_ref, zu_ref, w0, w1, w2, w3, dzg_ref, dzu_ref, own_ref, xp_ref, send_ref,
                wo_ref, acc, sem):
    step = pl.program_id(0)
    hw = FF // 2

    @pl.when(step == 0)
    def _():
        load_rows([((w0, w1, w2, w3), wo_ref)], sem)
        acc[...] = jnp.zeros_like(acc)

    dy = dy_ref[...]
    cw = 256
    h_t = h_ref[...].T
    n = hw // cw

    def dm_of(c):
        row0 = D + half * hw + c * cw
        return dot_nt(dy, wo_ref[row0:row0 + cw, :]).astype(BF16)

    for c in range(n):
        cols = slice(c * cw, (c + 1) * cw)
        dm = dm_of(c).astype(F32)
        g = zg_ref[:, cols].astype(F32)
        u = zu_ref[:, cols].astype(F32)
        sig = jax.nn.sigmoid(g)
        sl = g * sig
        dzu_ref[:, cols] = (dm * sl).astype(BF16)
        dzg_ref[:, cols] = (dm * u * (sig + sl * (1.0 - sig))).astype(BF16)
    acc[:, 0:hw] += dot(h_t, dzg_ref[...])
    acc[:, hw:2 * hw] += dot(h_t, dzu_ref[...])

    @pl.when(step == pl.num_programs(0) - 1)
    def _():
        store_grad_rows(acc, D // 4, own_ref, xp_ref, send_ref, sem, False)


def battn_kernel(chained, *refs):
    if chained:
        (dy_ref, h_ref, qkv_ref, c_ref, s_ref, w0, w1, w2, w3, _, in_own, in_xp, in_send,
         dz_ref, own_ref, xp_ref, send_ref, wo_ref, acc, sem) = refs
    else:
        (dy_ref, h_ref, qkv_ref, c_ref, s_ref, w0, w1, w2, w3,
         dz_ref, own_ref, xp_ref, send_ref, wo_ref, acc, sem) = refs
    step = pl.program_id(0)

    @pl.when(step == 0)
    def _():
        load_rows([((w0, w1, w2, w3), wo_ref)], sem)
        if chained:
            move_grad_rows(acc, D // 4, in_own, in_xp, in_send, sem, False, True)
        else:
            acc[...] = jnp.zeros_like(acc)

    do_all = dot_nt(dy_ref[...], wo_ref[0:D, :]).astype(BF16)
    lo = lane_iota((SEQ, 2 * HD)) < HD
    tri = tri_mask(128)
    trib = jnp.concatenate([tri] * 2, axis=1)
    for b in range(TOK // SEQ):
        r0 = b * SEQ
        zb = qkv_ref[r0:r0 + SEQ, :]
        do = do_all[r0:r0 + SEQ]
        k0, k1, v0, v1 = kv_tiles(zb[:, D:].astype(F32))
        kt0, kt1 = k0.T.astype(BF16), k1.T.astype(BF16)
        k0, k1, v0, v1 = [t.astype(BF16) for t in (k0, k1, v0, v1)]
        dk = [[None, None], [None, None]]
        dv = [[None, None], [None, None]]
        dq = [[None] * 4, [None] * 4]
        for blk in range(2):
            nk = (blk + 1) * HALF
            rows = slice(blk * HALF, (blk + 1) * HALF)
            k_st = jnp.concatenate([k0[:nk], k1[:nk]], axis=0)
            v_st = jnp.concatenate([v0[:nk], v1[:nk]], axis=0)
            k_t = jnp.concatenate([kt0[:, :nk], kt1[:, :nk]], axis=1)
            dk_b = dv_b = None
            for g in range(2):
                q = jnp.concatenate([zb[rows, (2 * g + i) * 128:(2 * g + i + 1) * 128] for i in range(2)], axis=0)
                dog = jnp.concatenate([do[rows, (2 * g + i) * 128:(2 * g + i + 1) * 128] for i in range(2)], axis=0)
                p = softmax_keys(dot_nt(k_st, q), nk, trib)
                dp = dot_nt(v_st, dog).astype(BF16)
                ds = []
                for i in range(2):
                    dph = [dp[i * nk + k * HALF:i * nk + (k + 1) * HALF].astype(F32) for k in range(nk // HALF)]
                    delta = sum(jnp.sum(a * c, axis=0, keepdims=True) for a, c in zip(dph, p[i]))
                    ds += [(c * (a - delta)).astype(BF16) for a, c in zip(dph, p[i])]
                ds = jnp.concatenate(ds, axis=0)
                pb = jnp.concatenate([t.astype(BF16) for ph in p for t in ph], axis=0)
                dv_g = dot(pb, dog)
                dk_g = dot(ds, q)
                dv_b = dv_g if dv_b is None else dv_b + dv_g
                dk_b = dk_g if dk_b is None else dk_b + dk_g
                dq_t = dot(k_t, ds).T
                for i in range(2):
                    dq[blk][2 * g + i] = dq_t[i * HALF:(i + 1) * HALF]
            for i in range(2):
                for k in range(nk // HALF):
                    sl = slice(i * nk + k * HALF, i * nk + (k + 1) * HALF)
                    dk[i][k] = dk_b[sl] if dk[i][k] is None else dk[i][k] + dk_b[sl]
                    dv[i][k] = dv_b[sl] if dv[i][k] is None else dv[i][k] + dv_b[sl]
        dk0, dk1, dv0, dv1 = [jnp.concatenate(t, axis=0) for t in (dk[0], dk[1], dv[0], dv[1])]
        kpart = dk0 + pltpu.roll(dk1, HD, 1)
        vpart = pltpu.roll(dv0, HD, 1) + dv1
        parts = [jnp.concatenate([dq[0][j], dq[1][j]], axis=0) for j in range(4)]
        parts.append(jnp.where(lo, kpart, vpart))
        for j in range(5):
            tc = slice(0, 128) if j < 4 else slice(128, 256)
            dr = parts[j].astype(BF16).astype(F32)
            dz_ref[r0:r0 + SEQ, j * 128:(j + 1) * 128] = (
                dr * c_ref[:, tc] - half_swap(dr) * s_ref[:, tc]).astype(BF16)
    acc[...] += dot_tn(h_ref[...], dz_ref[...])

    @pl.when(step == pl.num_programs(0) - 1)
    def _():
        store_grad_rows(acc, D // 4, own_ref, xp_ref, send_ref, sem, False)


def dx_kernel(x_ref, gain_ref, dy_ref, dzq_ref, dg0_ref, du0_ref, dg1_ref, du1_ref,
              q0, q1, q2, q3, w0, w1, w2, w3, *rest):
    dx_ref, dgain_ref, wq_ref, w_ref, sem = rest[-5:]
    step = pl.program_id(0)
    hw = FF // 2

    @pl.when(step == 0)
    def _():
        load_rows([((q0, q1, q2, q3), wq_ref), ((w0, w1, w2, w3), w_ref)], sem)
        dgain_ref[...] = jnp.zeros_like(dgain_ref)

    dh = dot_nt(dzq_ref[...], wq_ref[...])
    dh += dot_nt(dg0_ref[...], w_ref[:, 0:hw])
    dh += dot_nt(dg1_ref[...], w_ref[:, hw:2 * hw])
    dh += dot_nt(du0_ref[...], w_ref[:, 2 * hw:3 * hw])
    dh += dot_nt(du1_ref[...], w_ref[:, 3 * hw:4 * hw])
    dh = dh.astype(BF16).astype(F32)
    x = x_ref[...].astype(F32)
    cen = x - jnp.mean(x, axis=-1, keepdims=True)
    var = jnp.mean(cen * cen, axis=-1, keepdims=True)
    rstd = lax.rsqrt(var + 1e-6)
    xhat = cen * rstd
    dgain_ref[...] += jnp.sum(dh * xhat, axis=0, keepdims=True)
    dxh = dh * gain_ref[...]
    dx = rstd * (dxh - jnp.mean(dxh, axis=-1, keepdims=True)
                 - xhat * jnp.mean(dxh * xhat, axis=-1, keepdims=True))
    dx_ref[...] = (dy_ref[...].astype(F32) + dx.astype(BF16).astype(F32)).astype(BF16)


ANY = pl.BlockSpec(memory_space=pl.ANY)


def tok_spec(width, block=0, first=0):
    return pl.BlockSpec((TOK, width), lambda i: (i + first, block))


def full_spec(shape):
    return pl.BlockSpec(shape, lambda i: (0,) * len(shape))


def call(kernel, n_tok, in_specs, outs, out_specs, scratch, flops, nbytes, aliases=None):
    return pl.pallas_call(
        kernel,
        grid=(n_tok // TOK,),
        in_specs=in_specs,
        out_specs=out_specs,
        out_shape=[jax.ShapeDtypeStruct(s, t) for s, t in outs],
        scratch_shapes=scratch,
        input_output_aliases=aliases or {},
        compiler_params=pltpu.CompilerParams(
            dimension_semantics=("arbitrary",), vmem_limit_bytes=VMEM_LIMIT),
        cost_estimate=pl.CostEstimate(flops=int(flops), bytes_accessed=int(nbytes), transcendentals=0),
    )


def solution(mesh):
    batch_spec = P(("dp", "fsdp"), None, None)
    scale_spec = P(None, "fsdp")
    weight_spec = P(None, "fsdp", None)

    core_perm = [(0, 1), (1, 0), (2, 3), (3, 2)]
    x_perm = [(0, 2), (2, 0), (1, 3), (3, 1)]
    y_perm = [(0, 1), (1, 0)]

    def pp_core(a):
        return lax.ppermute(a, "fsdp", core_perm)

    def pp_x(a):
        return lax.ppermute(a, "fsdp", x_perm)

    def pp_y(a):
        return lax.ppermute(a, "dp", y_perm)

    def gather4(a):
        far = pp_x(a)
        return (a, pp_core(a), far, pp_core(far))

    def reduce4(own, xp, send):
        recv = pp_core(send)
        far = pp_x(xp + recv[1])
        mine = own + recv[0] + far
        return mine + pp_y(mine)

    def inner_step(x_in, grad_y, norm_scale, w_in, w_out):
        n_layers = w_in.shape[0]
        n_batch = x_in.shape[0]
        n_tok = n_batch * SEQ

        half = HD // 2
        inv_freq = 10000.0 ** (-(jnp.arange(half, dtype=F32) * 2.0 / HD))
        angles = jnp.arange(SEQ, dtype=F32)[:, None] * inv_freq[None, :]
        cos, sin = jnp.cos(angles), jnp.sin(angles)
        cos2 = jnp.concatenate([cos, cos], axis=1)
        sin2 = jnp.concatenate([-sin, sin], axis=1)
        qs = HD ** -0.5
        ones, zeros = jnp.ones_like(cos2), jnp.zeros_like(cos2)
        c_tab = jnp.concatenate([cos2 * qs, cos2 * qs, cos2, ones], axis=1)
        s_tab = jnp.concatenate([sin2 * qs, sin2 * qs, sin2, zeros], axis=1)

        q_pieces, g_pieces, o_pieces = [], [], []
        for l in range(n_layers):
            wq_l = w_in[l, :, :QKV]
            if l == 0:
                gcols = jnp.pad(norm_scale.T, ((0, 0), (0, 128 - n_layers)))
                wq_l = jnp.concatenate([wq_l, gcols], axis=1)
            q_pieces.append(gather4(wq_l))
            g_pieces.append(gather4(w_in[l, :, QKV:]))
            o_pieces.append(gather4(w_out[l]))
        gp = [a[:, QKV:QKV + n_layers].T for a in q_pieces[0]]
        own = owners()
        slot = jnp.arange(4)[None, :, None]
        gain = sum(jnp.where(slot == own[r], gp[r][:, None, :].astype(F32), 0.0) for r in range(4))
        gain = gain.reshape(n_layers, 1, D)

        x = x_in.reshape(n_tok, D)
        mm = 2.0 * n_tok * D
        saved = []
        sem = pltpu.SemaphoreType.DMA
        for l in range(n_layers):
            h, qkv, o = call(
                fwd_attn_kernel, n_tok,
                [tok_spec(D), full_spec((1, D)), full_spec((SEQ, 256)), full_spec((SEQ, 256))] + [ANY] * 4,
                [((n_tok, D), BF16), ((n_tok, QKV), BF16), ((n_tok, D), BF16)],
                [tok_spec(D), tok_spec(QKV), tok_spec(D)],
                [pltpu.VMEM((D, QKV), BF16), sem((4,))],
                mm * 2600, n_tok * D * 8,
            )(x, gain[l], c_tab, s_tab, *q_pieces[l])
            z, m, y = call(
                fwd_mlp_kernel, n_tok,
                [tok_spec(D), tok_spec(D), tok_spec(D)] + [ANY] * 8,
                [((n_tok, 2 * FF), BF16), ((n_tok, FF), BF16), ((n_tok, D), BF16)],
                [tok_spec(2 * FF), tok_spec(FF), tok_spec(D)],
                [pltpu.VMEM((D, 2 * FF), BF16), pltpu.VMEM((D + FF, D), BF16), sem((8,))],
                mm * 6700, n_tok * D * 32,
            )(x, h, o, *g_pieces[l], *o_pieces[l])
            saved.append((x, h, qkv, o, z, m))
            x = y

        dy = grad_y.reshape(n_tok, D)
        d_gain = [None] * n_layers
        d_win = [None] * n_layers
        d_wout = [None] * n_layers
        q4 = (D + FF) // 4

        def grad_outs(shape):
            return [(shape, F32), (shape, F32), ((2,) + shape, F32)]

        for l in reversed(range(n_layers)):
            xl, h, qkv, o, z, m = saved[l]
            g = call(
                dwo_kernel, n_tok, [tok_spec(D), tok_spec(D), tok_spec(FF)],
                grad_outs((D, q4)), [ANY] * 3,
                [pltpu.VMEM((D, D + FF), F32), sem((4,))],
                mm * 2560, n_tok * D * 12,
            )(dy, o, m)
            d_wout[l] = reduce4(*g).T
            hw = FF // 2
            dzs, win_parts = [], []
            for hf in range(2):
                dg, du, *g = call(
                    functools.partial(bmlp_kernel, hf), n_tok,
                    [tok_spec(D), tok_spec(D), tok_spec(hw, hf), tok_spec(hw, 2 + hf)] + [ANY] * 4,
                    [((n_tok, hw), BF16), ((n_tok, hw), BF16)] + grad_outs((D // 4, 2 * hw)),
                    [tok_spec(hw), tok_spec(hw)] + [ANY] * 3,
                    [pltpu.VMEM((D + FF, D), BF16), pltpu.VMEM((D, 2 * hw), F32), sem((4,))],
                    mm * 3072, n_tok * D * 20,
                )(dy, h, z, z, *o_pieces[l])
                dzs += [dg, du]
                win_parts.append(reduce4(*g))
            n_part = 2 if l == 0 else 1
            n_sub = n_tok // n_part
            dzq, g = None, ()
            for part in range(n_part):
                f0 = part * n_sub // TOK
                prev = (dzq, *g) if part else ()
                dzq, *g = call(
                    functools.partial(battn_kernel, part > 0), n_sub,
                    [tok_spec(D, 0, f0), tok_spec(D, 0, f0), tok_spec(QKV, 0, f0), full_spec((SEQ, 256)),
                     full_spec((SEQ, 256))] + [ANY] * (4 + len(prev)),
                    [((n_tok, QKV), BF16)] + grad_outs((D // 4, QKV)),
                    [tok_spec(QKV, 0, f0)] + [ANY] * 3,
                    [pltpu.VMEM((D + FF, D), BF16), pltpu.VMEM((D, QKV), F32), sem((4,))],
                    mm * 6200 / n_part, n_tok * D * 10 / n_part,
                    {9: 0} if part else None,
                )(dy, h, qkv, c_tab, s_tab, *o_pieces[l], *prev)
            wq = reduce4(*g)
            p0, p1 = win_parts
            d_win[l] = jnp.concatenate([wq, p0[:, :hw], p1[:, :hw], p0[:, hw:], p1[:, hw:]], axis=1)
            dx, gains = None, []
            for part in range(n_part):
                f0 = part * n_sub // TOK
                prev = (dx,) if part else ()
                dx, d_g = call(
                    dx_kernel, n_sub,
                    [tok_spec(D, 0, f0), full_spec((1, D)), tok_spec(D, 0, f0), tok_spec(QKV, 0, f0)]
                    + [tok_spec(hw, 0, f0)] * 4 + [ANY] * (8 + len(prev)),
                    [((n_tok, D), BF16), ((1, D), F32)],
                    [tok_spec(D, 0, f0), full_spec((1, D))],
                    [pltpu.VMEM((D, QKV), BF16), pltpu.VMEM((D, 2 * FF), BF16), sem((8,))],
                    mm * 4736 / n_part, n_tok * D * 20 / n_part,
                    {16: 0} if part else None,
                )(xl, gain[l], dy, dzq, *dzs, *q_pieces[l], *g_pieces[l], *prev)
                gains.append(d_g)
            dy = dx
            d_gain[l] = sum(gains)

        gg = jnp.concatenate(d_gain, axis=0)
        gg = gg + pp_core(gg)
        gg = gg + pp_x(gg)
        gg = gg + pp_y(gg)
        gg = lax.dynamic_slice(gg, (0, lax.axis_index("fsdp") * (D // 4)), (n_layers, D // 4))
        return (x.reshape(x_in.shape), dy.reshape(x_in.shape), gg, jnp.stack(d_win), jnp.stack(d_wout))

    return jax.shard_map(
        inner_step,
        mesh=mesh,
        in_specs=(batch_spec, batch_spec, scale_spec, weight_spec, weight_spec),
        out_specs=(batch_spec, batch_spec, scale_spec, weight_spec, weight_spec),
        check_vma=False,
    )
```

```python
import functools
import jax
import numpy as np
import jax.numpy as jnp
from jax import lax
from jax.experimental import pallas as pl
from jax.experimental.pallas import tpu as pltpu
from jax.sharding import PartitionSpec as P

F32 = jnp.float32
BF16 = jnp.bfloat16
SEQ = 256
HD = 64
D = 512
FF = 2048
QKV = D + 2 * HD
NEG = -1e30
VMEM_LIMIT = 60 * 1024 * 1024

TOK = 512


def dot(a, b):
    return jnp.dot(a, b, preferred_element_type=F32)


def dot_nt(a, b):
    return lax.dot_general(a, b, (((1,), (1,)), ((), ())), preferred_element_type=F32)


def dot_tn(a, b):
    return lax.dot_general(a, b, (((0,), (0,)), ((), ())), preferred_element_type=F32)


def owners():
    me = lax.axis_index("fsdp")
    x = me // 2
    c = me - 2 * x
    return [2 * x + c, 2 * x + (1 - c), 2 * (1 - x) + c, 2 * (1 - x) + (1 - c)]


def load_rows(groups, sem):
    own = owners()
    copies = []
    for pieces, dst in groups:
        rows = pieces[0].shape[0]
        for r in range(4):
            start = pl.multiple_of(own[r] * rows, rows)
            src = pieces[r].at[:, pl.ds(0, dst.shape[1])]
            cp = pltpu.make_async_copy(src, dst.at[pl.ds(start, rows), :], sem.at[len(copies)])
            cp.start()
            copies.append(cp)
    for cp in copies:
        cp.wait()


def lane_iota(shape):
    return lax.broadcasted_iota(jnp.int32, shape, len(shape) - 1)


def half_swap(z):
    n = z.shape[-1]
    lo = lax.rem(lane_iota(z.shape), HD) < HD // 2
    return jnp.where(lo, pltpu.roll(z, n - HD // 2, 1), pltpu.roll(z, HD // 2, 1))


HALF = SEQ // 2


def kv_tiles(kv):
    lo = lane_iota(kv.shape) < HD
    rolled = pltpu.roll(kv, HD, 1)
    zero = jnp.zeros_like(kv)
    return (jnp.where(lo, kv, zero), jnp.where(lo, zero, rolled),
            jnp.where(lo, rolled, zero), jnp.where(lo, zero, kv))


def tri_mask(n):
    key = lax.broadcasted_iota(jnp.int32, (HALF, n), 0)
    query = lax.rem(lax.broadcasted_iota(jnp.int32, (HALF, n), 1), HALF)
    return query >= key


def softmax_keys(s, n_keys, tri):
    out = []
    for i in range(2):
        sh = s[i * n_keys:(i + 1) * n_keys]
        sh = [sh[k * HALF:(k + 1) * HALF] for k in range(n_keys // HALF)]
        sh[-1] = jnp.where(tri, sh[-1], NEG)
        m = jnp.max(sh[-1], axis=0, keepdims=True)
        for t in sh[:-1]:
            m = jnp.maximum(m, jnp.max(t, axis=0, keepdims=True))
        e = [jnp.exp(t - m) for t in sh]
        l = jnp.sum(e[0], axis=0, keepdims=True)
        for t in e[1:]:
            l = l + jnp.sum(t, axis=0, keepdims=True)
        inv = 1.0 / l
        out.append([t * inv for t in e])
    return out


def expand_tables(cs_ref, c_ref, s_ref):
    cs = cs_ref[...]
    lo = lane_iota(cs.shape) < HD
    rolled = pltpu.roll(cs, HD, 1)
    cos = jnp.where(lo, cs, rolled)
    sin = jnp.where(lo, rolled, cs)
    c_ref[:, 0:128] = cos * HD ** -0.5
    s_ref[:, 0:128] = sin * HD ** -0.5
    c_ref[:, 128:256] = jnp.where(lo, cos, 1.0)
    s_ref[:, 128:256] = jnp.where(lo, sin, 0.0)


def rotary_table():
    half = HD // 2
    inv_freq = np.float32(10000.0) ** (-(np.arange(half, dtype=np.float32) * np.float32(2.0 / HD)))
    angles = np.arange(SEQ, dtype=np.float32)[:, None] * inv_freq[None, :]
    cos, sin = np.cos(angles), np.sin(angles)
    return np.concatenate([cos, cos, -sin, sin], axis=1).astype(np.float32)


def fwd_attn_kernel(x_ref, gain_ref, cs_ref, w0, w1, w2, w3, h_ref, qkv_ref, o_ref, w_ref, c_ref, s_ref, sem):
    @pl.when(pl.program_id(0) == 0)
    def _():
        expand_tables(cs_ref, c_ref, s_ref)
        load_rows([((w0, w1, w2, w3), w_ref)], sem)

    x = x_ref[...].astype(F32)
    cen = x - jnp.mean(x, axis=-1, keepdims=True)
    var = jnp.mean(cen * cen, axis=-1, keepdims=True)
    h = (cen * lax.rsqrt(var + 1e-6) * gain_ref[...]).astype(BF16)
    h_ref[...] = h
    z_all = dot(h, w_ref[...]).astype(BF16)
    tri = tri_mask(128)
    for b in range(TOK // SEQ):
        r0 = b * SEQ
        zt = []
        for j in range(5):
            t = z_all[r0:r0 + SEQ, j * 128:(j + 1) * 128].astype(F32)
            tc = slice(0, 128) if j < 4 else slice(128, 256)
            t = (t * c_ref[:, tc] + half_swap(t) * s_ref[:, tc]).astype(BF16)
            qkv_ref[r0:r0 + SEQ, j * 128:(j + 1) * 128] = t
            zt.append(t)
        k0, k1, v0, v1 = kv_tiles(zt[4].astype(F32))
        k0, k1 = k0.astype(BF16), k1.astype(BF16)
        v0, v1 = v0.T.astype(BF16), v1.T.astype(BF16)
        for blk in range(2):
            nk = (blk + 1) * HALF
            rows = slice(blk * HALF, (blk + 1) * HALF)
            k_st = jnp.concatenate([k0[:nk], k1[:nk]], axis=0)
            v_t = jnp.concatenate([v0[:, :nk], v1[:, :nk]], axis=1)
            for g in range(2):
                q = jnp.concatenate([zt[2 * g + i][rows] for i in range(2)], axis=0)
                s = dot_nt(k_st, q)
                trib = jnp.concatenate([tri] * 2, axis=1)
                p = softmax_keys(s, nk, trib)
                pb = jnp.concatenate([t.astype(BF16) for ph in p for t in ph], axis=0)
                o = dot(v_t, pb).T.astype(BF16)
                for i in range(2):
                    j = 2 * g + i
                    o_ref[r0 + blk * HALF:r0 + (blk + 1) * HALF, j * 128:(j + 1) * 128] = o[i * HALF:(i + 1) * HALF]


def fwd_mlp_kernel(x_ref, h_ref, o_ref, g0, g1, g2, g3, u0, u1, u2, u3, z_ref, m_ref, y_ref, w_ref, wo_ref, sem):
    @pl.when(pl.program_id(0) == 0)
    def _():
        load_rows([((g0, g1, g2, g3), w_ref), ((u0, u1, u2, u3), wo_ref)], sem)

    h = h_ref[...]
    cw = 512
    acc = dot(o_ref[...], wo_ref[0:D, :])
    for c in range(FF // cw):
        gc = slice(c * cw, (c + 1) * cw)
        uc = slice(FF + c * cw, FF + (c + 1) * cw)
        g = dot(h, w_ref[:, gc]).astype(BF16)
        u = dot(h, w_ref[:, uc]).astype(BF16)
        z_ref[:, gc] = g
        z_ref[:, uc] = u
        g = g.astype(F32)
        m = (g * jax.nn.sigmoid(g) * u.astype(F32)).astype(BF16)
        m_ref[:, gc] = m
        acc = acc + dot(m, wo_ref[D + c * cw:D + (c + 1) * cw, :])
    y_ref[...] = (x_ref[...].astype(F32) + acc).astype(BF16)


def store_grad_rows(acc, width, own_ref, xp_ref, send_ref, sem, by_cols):
    own = owners()
    copies = []
    for r, dst in enumerate((own_ref, send_ref.at[0], xp_ref, send_ref.at[1])):
        start = pl.multiple_of(own[r] * width, 128)
        src = acc.at[:, pl.ds(start, width)] if by_cols else acc.at[pl.ds(start, width), :]
        cp = pltpu.make_async_copy(src, dst, sem.at[r])
        cp.start()
        copies.append(cp)
    for cp in copies:
        cp.wait()


def dwo_kernel(dy_ref, o_ref, m_ref, own_ref, xp_ref, send_ref, acc, sem):
    step = pl.program_id(0)

    @pl.when(step == 0)
    def _():
        acc[...] = jnp.zeros_like(acc)

    dy = dy_ref[...]
    acc[:, 0:D] += dot_tn(dy, o_ref[...])
    cw = 512
    for c in range(FF // cw):
        acc[:, D + c * cw:D + (c + 1) * cw] += dot_tn(dy, m_ref[:, c * cw:(c + 1) * cw])

    @pl.when(step == pl.num_programs(0) - 1)
    def _():
        store_grad_rows(acc, (D + FF) // 4, own_ref, xp_ref, send_ref, sem, True)


def mlp_grads(dy, h_t, wo_ref, row_base, zg_ref, zu_ref, dzg_ref, dzu_ref, acc, width, cw, side=None):
    def dz_of(c):
        cols = slice(c * cw, (c + 1) * cw)
        rows = slice(row_base + c * cw, row_base + (c + 1) * cw)
        dm = dot_nt(dy, wo_ref[rows, :]).astype(BF16).astype(F32)
        g = zg_ref[:, cols].astype(F32)
        u = zu_ref[:, cols].astype(F32)
        sig = jax.nn.sigmoid(g)
        sl = g * sig
        du = (dm * sl).astype(BF16)
        dg = (dm * u * (sig + sl * (1.0 - sig))).astype(BF16)
        dzu_ref[:, cols] = du
        dzg_ref[:, cols] = dg
        return dg, du

    def add_dw(c, parts):
        dg, du = parts
        acc[:, c * cw:(c + 1) * cw] += dot(h_t, dg)
        acc[:, width + c * cw:width + (c + 1) * cw] += dot(h_t, du)

    n = width // cw
    prev = dz_of(0)
    for c in range(n):
        nxt = dz_of(c + 1) if c + 1 < n else None
        if side is not None:
            side(c)
        add_dw(c, prev)
        prev = nxt


def bmlp_kernel(half, dy_ref, h_ref, zg_ref, zu_ref, w0, w1, w2, w3, dzg_ref, dzu_ref, own_ref, xp_ref, send_ref,
                wo_ref, acc, sem):
    step = pl.program_id(0)
    hw = FF // 2

    @pl.when(step == 0)
    def _():
        load_rows([((w0, w1, w2, w3), wo_ref)], sem)
        acc[...] = jnp.zeros_like(acc)

    mlp_grads(dy_ref[...], h_ref[...].T, wo_ref, D + half * hw, zg_ref, zu_ref, dzg_ref, dzu_ref, acc, hw, 256)

    @pl.when(step == pl.num_programs(0) - 1)
    def _():
        store_grad_rows(acc, D // 4, own_ref, xp_ref, send_ref, sem, False)


def bmlp_dwo_kernel(dy_ref, h_ref, o_ref, m_ref, zg_ref, zu_ref, w0, w1, w2, w3, dzg_ref, dzu_ref,
                    oo_ref, ox_ref, os_ref, own_ref, xp_ref, send_ref, wo_ref, acc_o, acc, sem):
    step = pl.program_id(0)

    @pl.when(step == 0)
    def _():
        load_rows([((w0, w1, w2, w3), wo_ref)], sem)
        acc[...] = jnp.zeros_like(acc)
        acc_o[...] = jnp.zeros_like(acc_o)

    dy = dy_ref[...]
    dy_t = dy.T
    cw = 256

    def side(c):
        acc_o[:, D + c * cw:D + (c + 1) * cw] += dot(dy_t, m_ref[:, c * cw:(c + 1) * cw])

    acc_o[:, 0:D] += dot(dy_t, o_ref[...])
    mlp_grads(dy, h_ref[...].T, wo_ref, D, zg_ref, zu_ref, dzg_ref, dzu_ref, acc, FF, cw, side)

    @pl.when(step == pl.num_programs(0) - 1)
    def _():
        store_grad_rows(acc_o, (D + FF) // 4, oo_ref, ox_ref, os_ref, sem, True)
        store_grad_rows(acc, D // 4, own_ref, xp_ref, send_ref, sem, False)


def battn_kernel(dy_ref, h_ref, qkv_ref, cs_ref, w0, w1, w2, w3, dz_ref, own_ref, xp_ref, send_ref,
                 wo_ref, acc, c_ref, s_ref, sem):
    step = pl.program_id(0)

    @pl.when(step == 0)
    def _():
        load_rows([((w0, w1, w2, w3), wo_ref)], sem)
        expand_tables(cs_ref, c_ref, s_ref)
        acc[...] = jnp.zeros_like(acc)

    do_all = dot_nt(dy_ref[...], wo_ref[0:D, :]).astype(BF16)
    lo = lane_iota((SEQ, 2 * HD)) < HD
    tri = tri_mask(128)
    trib = jnp.concatenate([tri] * 2, axis=1)
    for b in range(TOK // SEQ):
        r0 = b * SEQ
        zb = qkv_ref[r0:r0 + SEQ, :]
        do = do_all[r0:r0 + SEQ]
        k0, k1, v0, v1 = kv_tiles(zb[:, D:].astype(F32))
        kt0, kt1 = k0.T.astype(BF16), k1.T.astype(BF16)
        k0, k1, v0, v1 = [t.astype(BF16) for t in (k0, k1, v0, v1)]
        dk = [[None, None], [None, None]]
        dv = [[None, None], [None, None]]
        dq = [[None] * 4, [None] * 4]
        for blk in range(2):
            nk = (blk + 1) * HALF
            rows = slice(blk * HALF, (blk + 1) * HALF)
            k_st = jnp.concatenate([k0[:nk], k1[:nk]], axis=0)
            v_st = jnp.concatenate([v0[:nk], v1[:nk]], axis=0)
            k_t = jnp.concatenate([kt0[:, :nk], kt1[:, :nk]], axis=1)
            dk_b = dv_b = None
            for g in range(2):
                q = jnp.concatenate([zb[rows, (2 * g + i) * 128:(2 * g + i + 1) * 128] for i in range(2)], axis=0)
                dog = jnp.concatenate([do[rows, (2 * g + i) * 128:(2 * g + i + 1) * 128] for i in range(2)], axis=0)
                p = softmax_keys(dot_nt(k_st, q), nk, trib)
                dp = dot_nt(v_st, dog).astype(BF16)
                ds = []
                for i in range(2):
                    dph = [dp[i * nk + k * HALF:i * nk + (k + 1) * HALF].astype(F32) for k in range(nk // HALF)]
                    delta = sum(jnp.sum(a * c, axis=0, keepdims=True) for a, c in zip(dph, p[i]))
                    ds += [(c * (a - delta)).astype(BF16) for a, c in zip(dph, p[i])]
                ds = jnp.concatenate(ds, axis=0)
                pb = jnp.concatenate([t.astype(BF16) for ph in p for t in ph], axis=0)
                dv_g = dot(pb, dog)
                dk_g = dot(ds, q)
                dv_b = dv_g if dv_b is None else dv_b + dv_g
                dk_b = dk_g if dk_b is None else dk_b + dk_g
                dq_t = dot(k_t, ds).T
                for i in range(2):
                    dq[blk][2 * g + i] = dq_t[i * HALF:(i + 1) * HALF]
            for i in range(2):
                for k in range(nk // HALF):
                    sl = slice(i * nk + k * HALF, i * nk + (k + 1) * HALF)
                    dk[i][k] = dk_b[sl] if dk[i][k] is None else dk[i][k] + dk_b[sl]
                    dv[i][k] = dv_b[sl] if dv[i][k] is None else dv[i][k] + dv_b[sl]
        dk0, dk1, dv0, dv1 = [jnp.concatenate(t, axis=0) for t in (dk[0], dk[1], dv[0], dv[1])]
        kpart = dk0 + pltpu.roll(dk1, HD, 1)
        vpart = pltpu.roll(dv0, HD, 1) + dv1
        parts = [jnp.concatenate([dq[0][j], dq[1][j]], axis=0) for j in range(4)]
        parts.append(jnp.where(lo, kpart, vpart))
        for j in range(5):
            tc = slice(0, 128) if j < 4 else slice(128, 256)
            dr = parts[j].astype(BF16).astype(F32)
            dz_ref[r0:r0 + SEQ, j * 128:(j + 1) * 128] = (
                dr * c_ref[:, tc] - half_swap(dr) * s_ref[:, tc]).astype(BF16)
    acc[...] += dot_tn(h_ref[...], dz_ref[...])

    @pl.when(step == pl.num_programs(0) - 1)
    def _():
        store_grad_rows(acc, D // 4, own_ref, xp_ref, send_ref, sem, False)


def dx_kernel(spans, x_ref, gain_ref, dy_ref, dzq_ref, *refs):
    dz_refs = refs[:len(spans)]
    q0, q1, q2, q3, w0, w1, w2, w3, dx_ref, dgain_ref, wq_ref, w_ref, sem = refs[len(spans):]
    step = pl.program_id(0)

    @pl.when(step == 0)
    def _():
        load_rows([((q0, q1, q2, q3), wq_ref), ((w0, w1, w2, w3), w_ref)], sem)
        dgain_ref[...] = jnp.zeros_like(dgain_ref)

    dh = dot_nt(dzq_ref[...], wq_ref[...])
    for (start, width), dz_ref in zip(spans, dz_refs):
        dh += dot_nt(dz_ref[...], w_ref[:, start:start + width])
    dh = dh.astype(BF16).astype(F32)
    x = x_ref[...].astype(F32)
    cen = x - jnp.mean(x, axis=-1, keepdims=True)
    var = jnp.mean(cen * cen, axis=-1, keepdims=True)
    rstd = lax.rsqrt(var + 1e-6)
    xhat = cen * rstd
    dgain_ref[...] += jnp.sum(dh * xhat, axis=0, keepdims=True)
    dxh = dh * gain_ref[...]
    dx = rstd * (dxh - jnp.mean(dxh, axis=-1, keepdims=True)
                 - xhat * jnp.mean(dxh * xhat, axis=-1, keepdims=True))
    dx_ref[...] = (dy_ref[...].astype(F32) + dx.astype(BF16).astype(F32)).astype(BF16)


ANY = pl.BlockSpec(memory_space=pl.ANY)


def tok_spec(width, block=0, first=0):
    return pl.BlockSpec((TOK, width), lambda i: (i + first, block))


def full_spec(shape):
    return pl.BlockSpec(shape, lambda i: (0,) * len(shape))


def call(kernel, n_tok, in_specs, outs, out_specs, scratch, flops, nbytes, aliases=None):
    return pl.pallas_call(
        kernel,
        grid=(n_tok // TOK,),
        in_specs=in_specs,
        out_specs=out_specs,
        out_shape=[jax.ShapeDtypeStruct(s, t) for s, t in outs],
        scratch_shapes=scratch,
        input_output_aliases=aliases or {},
        compiler_params=pltpu.CompilerParams(
            dimension_semantics=("arbitrary",), vmem_limit_bytes=VMEM_LIMIT),
        cost_estimate=pl.CostEstimate(flops=int(flops), bytes_accessed=int(nbytes), transcendentals=0),
    )


def solution(mesh):
    batch_spec = P(("dp", "fsdp"), None, None)
    scale_spec = P(None, "fsdp")
    weight_spec = P(None, "fsdp", None)

    core_perm = [(0, 1), (1, 0), (2, 3), (3, 2)]
    x_perm = [(0, 2), (2, 0), (1, 3), (3, 1)]
    y_perm = [(0, 1), (1, 0)]

    def pp_core(a):
        return lax.ppermute(a, "fsdp", core_perm)

    def pp_x(a):
        return lax.ppermute(a, "fsdp", x_perm)

    def pp_y(a):
        return lax.ppermute(a, "dp", y_perm)

    def gather4(a):
        far = pp_x(a)
        return (a, pp_core(a), far, pp_core(far))

    def reduce4(own, xp, send):
        recv = pp_core(send)
        far = pp_x(xp + recv[1])
        mine = own + recv[0] + far
        return mine + pp_y(mine)

    def inner_step(x_in, grad_y, norm_scale, w_in, w_out):
        n_layers = w_in.shape[0]
        n_batch = x_in.shape[0]
        n_tok = n_batch * SEQ

        cs_tab = jnp.asarray(rotary_table())

        q_pieces, g_pieces, o_pieces = [], [], []
        for l in range(n_layers):
            wq_l = w_in[l, :, :QKV]
            if l == 0:
                gcols = jnp.pad(norm_scale.T, ((0, 0), (0, 128 - n_layers)))
                wq_l = jnp.concatenate([wq_l, gcols], axis=1)
            q_pieces.append(gather4(wq_l))
            g_pieces.append(gather4(w_in[l, :, QKV:]))
            o_pieces.append(gather4(w_out[l]))
        gp = [a[:, QKV:QKV + n_layers].T for a in q_pieces[0]]
        own = owners()
        slot = jnp.arange(4)[None, :, None]
        gain = sum(jnp.where(slot == own[r], gp[r][:, None, :].astype(F32), 0.0) for r in range(4))
        gain = gain.reshape(n_layers, 1, D)

        x = x_in.reshape(n_tok, D)
        mm = 2.0 * n_tok * D
        saved = []
        sem = pltpu.SemaphoreType.DMA
        for l in range(n_layers):
            h, qkv, o = call(
                fwd_attn_kernel, n_tok,
                [tok_spec(D), full_spec((1, D)), full_spec((SEQ, 128))] + [ANY] * 4,
                [((n_tok, D), BF16), ((n_tok, QKV), BF16), ((n_tok, D), BF16)],
                [tok_spec(D), tok_spec(QKV), tok_spec(D)],
                [pltpu.VMEM((D, QKV), BF16), pltpu.VMEM((SEQ, 256), F32), pltpu.VMEM((SEQ, 256), F32), sem((4,))],
                mm * 2600, n_tok * D * 8,
            )(x, gain[l], cs_tab, *q_pieces[l])
            z, m, y = call(
                fwd_mlp_kernel, n_tok,
                [tok_spec(D), tok_spec(D), tok_spec(D)] + [ANY] * 8,
                [((n_tok, 2 * FF), BF16), ((n_tok, FF), BF16), ((n_tok, D), BF16)],
                [tok_spec(2 * FF), tok_spec(FF), tok_spec(D)],
                [pltpu.VMEM((D, 2 * FF), BF16), pltpu.VMEM((D + FF, D), BF16), sem((8,))],
                mm * 6700, n_tok * D * 32,
            )(x, h, o, *g_pieces[l], *o_pieces[l])
            saved.append((x, h, qkv, o, z, m))
            x = y

        dy = grad_y.reshape(n_tok, D)
        d_gain = [None] * n_layers
        d_win = [None] * n_layers
        d_wout = [None] * n_layers
        q4 = (D + FF) // 4

        def grad_outs(shape):
            return [(shape, F32), (shape, F32), ((2,) + shape, F32)]

        for l in reversed(range(n_layers)):
            xl, h, qkv, o, z, m = saved[l]
            hw = FF // 2
            n_half = 2 if l == 0 else 1
            fw = FF // n_half
            dzs, spans, win_parts = [], [], []
            if n_half == 1:
                dg, du, *g = call(
                    bmlp_dwo_kernel, n_tok,
                    [tok_spec(D)] * 3 + [tok_spec(FF), tok_spec(FF, 0), tok_spec(FF, 1)] + [ANY] * 4,
                    [((n_tok, FF), BF16), ((n_tok, FF), BF16)] + grad_outs((D, q4)) + grad_outs((D // 4, 2 * FF)),
                    [tok_spec(FF), tok_spec(FF)] + [ANY] * 6,
                    [pltpu.VMEM((D + FF, D), BF16), pltpu.VMEM((D, D + FF), F32), pltpu.VMEM((D, 2 * FF), F32),
                     sem((4,))],
                    mm * 8704, n_tok * D * 50,
                )(dy, h, o, m, z, z, *o_pieces[l])
                dzs, spans = [dg, du], [(0, FF), (FF, FF)]
                d_wout[l] = reduce4(*g[:3]).T
                win_parts.append(reduce4(*g[3:]))
            else:
                g = call(
                    dwo_kernel, n_tok, [tok_spec(D), tok_spec(D), tok_spec(FF)],
                    grad_outs((D, q4)), [ANY] * 3,
                    [pltpu.VMEM((D, D + FF), F32), sem((4,))],
                    mm * 2560, n_tok * D * 12,
                )(dy, o, m)
                d_wout[l] = reduce4(*g).T
                for hf in range(2):
                    dg, du, *g = call(
                        functools.partial(bmlp_kernel, hf), n_tok,
                        [tok_spec(D), tok_spec(D), tok_spec(hw, hf), tok_spec(hw, 2 + hf)] + [ANY] * 4,
                        [((n_tok, hw), BF16), ((n_tok, hw), BF16)] + grad_outs((D // 4, 2 * hw)),
                        [tok_spec(hw), tok_spec(hw)] + [ANY] * 3,
                        [pltpu.VMEM((D + FF, D), BF16), pltpu.VMEM((D, 2 * hw), F32), sem((4,))],
                        mm * 3072, n_tok * D * 20,
                    )(dy, h, z, z, *o_pieces[l])
                    dzs += [dg, du]
                    spans += [(hf * hw, hw), (FF + hf * hw, hw)]
                    win_parts.append(reduce4(*g))
            dzq, *g = call(
                battn_kernel, n_tok,
                [tok_spec(D), tok_spec(D), tok_spec(QKV), full_spec((SEQ, 128))] + [ANY] * 4,
                [((n_tok, QKV), BF16)] + grad_outs((D // 4, QKV)),
                [tok_spec(QKV)] + [ANY] * 3,
                [pltpu.VMEM((D + FF, D), BF16), pltpu.VMEM((D, QKV), F32), pltpu.VMEM((SEQ, 256), F32),
                 pltpu.VMEM((SEQ, 256), F32), sem((4,))],
                mm * 6200, n_tok * D * 10,
            )(dy, h, qkv, cs_tab, *o_pieces[l])
            wq = reduce4(*g)
            d_win[l] = jnp.concatenate(
                [wq] + [p[:, :fw] for p in win_parts] + [p[:, fw:] for p in win_parts], axis=1)
            dy, d_gain[l] = call(
                functools.partial(dx_kernel, tuple(spans)), n_tok,
                [tok_spec(D), full_spec((1, D)), tok_spec(D), tok_spec(QKV)] + [tok_spec(fw)] * len(dzs) + [ANY] * 8,
                [((n_tok, D), BF16), ((1, D), F32)],
                [tok_spec(D), full_spec((1, D))],
                [pltpu.VMEM((D, QKV), BF16), pltpu.VMEM((D, 2 * FF), BF16), sem((8,))],
                mm * 4736, n_tok * D * 20,
            )(xl, gain[l], dy, dzq, *dzs, *q_pieces[l], *g_pieces[l])

        gg = jnp.concatenate(d_gain, axis=0)
        gg = gg + pp_core(gg)
        gg = gg + pp_x(gg)
        gg = gg + pp_y(gg)
        gg = lax.dynamic_slice(gg, (0, lax.axis_index("fsdp") * (D // 4)), (n_layers, D // 4))
        return (x.reshape(x_in.shape), dy.reshape(x_in.shape), gg, jnp.stack(d_win), jnp.stack(d_wout))

    return jax.shard_map(
        inner_step,
        mesh=mesh,
        in_specs=(batch_spec, batch_spec, scale_spec, weight_spec, weight_spec),
        out_specs=(batch_spec, batch_spec, scale_spec, weight_spec, weight_spec),
        check_vma=False,
    )
```

```python
import functools
import jax
import numpy as np
import jax.numpy as jnp
from jax import lax
from jax.experimental import pallas as pl
from jax.experimental.pallas import tpu as pltpu
from jax.sharding import PartitionSpec as P

F32 = jnp.float32
BF16 = jnp.bfloat16
SEQ = 256
HD = 64
D = 512
FF = 2048
QKV = D + 2 * HD
NEG = -1e30
VMEM_LIMIT = 60 * 1024 * 1024

TOK = 512


def dot(a, b):
    return jnp.dot(a, b, preferred_element_type=F32)


def dot_nt(a, b):
    return lax.dot_general(a, b, (((1,), (1,)), ((), ())), preferred_element_type=F32)


def dot_tn(a, b):
    return lax.dot_general(a, b, (((0,), (0,)), ((), ())), preferred_element_type=F32)


def owners():
    me = lax.axis_index("fsdp")
    x = me // 2
    c = me - 2 * x
    return [2 * x + c, 2 * x + (1 - c), 2 * (1 - x) + c, 2 * (1 - x) + (1 - c)]


def start_rows(groups, sem):
    own = owners()
    copies = []
    for pieces, dst in groups:
        rows = pieces[0].shape[0]
        for r in range(4):
            start = pl.multiple_of(own[r] * rows, rows)
            src = pieces[r].at[:, pl.ds(0, dst.shape[1])]
            cp = pltpu.make_async_copy(src, dst.at[pl.ds(start, rows), :], sem.at[len(copies)])
            cp.start()
            copies.append(cp)
    return copies


def wait_all(copies):
    for cp in copies:
        cp.wait()


def lane_iota(shape):
    return lax.broadcasted_iota(jnp.int32, shape, len(shape) - 1)


def half_swap(z):
    n = z.shape[-1]
    lo = lax.rem(lane_iota(z.shape), HD) < HD // 2
    return jnp.where(lo, pltpu.roll(z, n - HD // 2, 1), pltpu.roll(z, HD // 2, 1))


HALF = SEQ // 2


def kv_tiles(kv):
    lo = lane_iota(kv.shape) < HD
    rolled = pltpu.roll(kv, HD, 1)
    zero = jnp.zeros_like(kv)
    return (jnp.where(lo, kv, zero), jnp.where(lo, zero, rolled),
            jnp.where(lo, rolled, zero), jnp.where(lo, zero, kv))


def tri_mask(n):
    key = lax.broadcasted_iota(jnp.int32, (HALF, n), 0)
    query = lax.rem(lax.broadcasted_iota(jnp.int32, (HALF, n), 1), HALF)
    return query >= key


def softmax_keys(s, n_keys, tri):
    out = []
    for i in range(2):
        sh = s[i * n_keys:(i + 1) * n_keys]
        sh = [sh[k * HALF:(k + 1) * HALF] for k in range(n_keys // HALF)]
        sh[-1] = jnp.where(tri, sh[-1], NEG)
        m = jnp.max(sh[-1], axis=0, keepdims=True)
        for t in sh[:-1]:
            m = jnp.maximum(m, jnp.max(t, axis=0, keepdims=True))
        e = [jnp.exp(t - m) for t in sh]
        l = jnp.sum(e[0], axis=0, keepdims=True)
        for t in e[1:]:
            l = l + jnp.sum(t, axis=0, keepdims=True)
        inv = 1.0 / l
        out.append([t * inv for t in e])
    return out


def expand_tables(cs_ref, c_ref, s_ref):
    cs = cs_ref[...]
    lo = lane_iota(cs.shape) < HD
    rolled = pltpu.roll(cs, HD, 1)
    cos = jnp.where(lo, cs, rolled)
    sin = jnp.where(lo, rolled, cs)
    c_ref[:, 0:128] = cos * HD ** -0.5
    s_ref[:, 0:128] = sin * HD ** -0.5
    c_ref[:, 128:256] = jnp.where(lo, cos, 1.0)
    s_ref[:, 128:256] = jnp.where(lo, sin, 0.0)


def rotary_table():
    half = HD // 2
    inv_freq = np.float32(10000.0) ** (-(np.arange(half, dtype=np.float32) * np.float32(2.0 / HD)))
    angles = np.arange(SEQ, dtype=np.float32)[:, None] * inv_freq[None, :]
    cos, sin = np.cos(angles), np.sin(angles)
    return np.concatenate([cos, cos, -sin, sin], axis=1).astype(np.float32)


def fwd_attn_kernel(x_ref, gain_ref, cs_ref, w0, w1, w2, w3, h_ref, qkv_ref, o_ref, w_ref, c_ref, s_ref, sem):
    @pl.when(pl.program_id(0) == 0)
    def _():
        copies = start_rows([((w0, w1, w2, w3), w_ref)], sem)
        expand_tables(cs_ref, c_ref, s_ref)
        wait_all(copies)

    x = x_ref[...].astype(F32)
    cen = x - jnp.mean(x, axis=-1, keepdims=True)
    var = jnp.mean(cen * cen, axis=-1, keepdims=True)
    h = (cen * lax.rsqrt(var + 1e-6) * gain_ref[...]).astype(BF16)
    h_ref[...] = h
    z_all = dot(h, w_ref[...]).astype(BF16)
    tri = tri_mask(128)
    for b in range(TOK // SEQ):
        r0 = b * SEQ
        zt = []
        for j in range(5):
            t = z_all[r0:r0 + SEQ, j * 128:(j + 1) * 128].astype(F32)
            tc = slice(0, 128) if j < 4 else slice(128, 256)
            t = (t * c_ref[:, tc] + half_swap(t) * s_ref[:, tc]).astype(BF16)
            qkv_ref[r0:r0 + SEQ, j * 128:(j + 1) * 128] = t
            zt.append(t)
        k0, k1, v0, v1 = kv_tiles(zt[4].astype(F32))
        k0, k1 = k0.astype(BF16), k1.astype(BF16)
        v0, v1 = v0.T.astype(BF16), v1.T.astype(BF16)
        for blk in range(2):
            nk = (blk + 1) * HALF
            rows = slice(blk * HALF, (blk + 1) * HALF)
            k_st = jnp.concatenate([k0[:nk], k1[:nk]], axis=0)
            v_t = jnp.concatenate([v0[:, :nk], v1[:, :nk]], axis=1)
            for g in range(2):
                q = jnp.concatenate([zt[2 * g + i][rows] for i in range(2)], axis=0)
                s = dot_nt(k_st, q)
                trib = jnp.concatenate([tri] * 2, axis=1)
                p = softmax_keys(s, nk, trib)
                pb = jnp.concatenate([t.astype(BF16) for ph in p for t in ph], axis=0)
                o = dot(v_t, pb).T.astype(BF16)
                for i in range(2):
                    j = 2 * g + i
                    o_ref[r0 + blk * HALF:r0 + (blk + 1) * HALF, j * 128:(j + 1) * 128] = o[i * HALF:(i + 1) * HALF]


def fwd_mlp_kernel(x_ref, h_ref, o_ref, g0, g1, g2, g3, u0, u1, u2, u3, z_ref, m_ref, y_ref, w_ref, wo_ref, sem):
    @pl.when(pl.program_id(0) == 0)
    def _():
        copies = start_rows([((g0, g1, g2, g3), w_ref), ((u0, u1, u2, u3), wo_ref)], sem)
        wait_all(copies)

    h = h_ref[...]
    cw = 512
    acc = dot(o_ref[...], wo_ref[0:D, :])
    for c in range(FF // cw):
        gc = slice(c * cw, (c + 1) * cw)
        uc = slice(FF + c * cw, FF + (c + 1) * cw)
        g = dot(h, w_ref[:, gc]).astype(BF16)
        u = dot(h, w_ref[:, uc]).astype(BF16)
        z_ref[:, gc] = g
        z_ref[:, uc] = u
        g = g.astype(F32)
        m = (g * jax.nn.sigmoid(g) * u.astype(F32)).astype(BF16)
        m_ref[:, gc] = m
        acc = acc + dot(m, wo_ref[D + c * cw:D + (c + 1) * cw, :])
    y_ref[...] = (x_ref[...].astype(F32) + acc).astype(BF16)


def start_grad_rows(acc, width, own_ref, xp_ref, send_ref, sem, by_cols, first=0):
    own = owners()
    copies = []
    for r, dst in ((1, send_ref.at[0]), (3, send_ref.at[1]), (0, own_ref), (2, xp_ref)):
        start = pl.multiple_of(own[r] * width, 128)
        src = acc.at[:, pl.ds(start, width)] if by_cols else acc.at[pl.ds(start, width), :]
        cp = pltpu.make_async_copy(src, dst, sem.at[first + r])
        cp.start()
        copies.append(cp)
    return copies


def store_grad_rows(*args):
    wait_all(start_grad_rows(*args))


def dwo_kernel(dy_ref, o_ref, m_ref, own_ref, xp_ref, send_ref, acc, sem):
    step = pl.program_id(0)

    @pl.when(step == 0)
    def _():
        acc[...] = jnp.zeros_like(acc)

    dy = dy_ref[...]
    acc[:, 0:D] += dot_tn(dy, o_ref[...])
    cw = 512
    for c in range(FF // cw):
        acc[:, D + c * cw:D + (c + 1) * cw] += dot_tn(dy, m_ref[:, c * cw:(c + 1) * cw])

    @pl.when(step == pl.num_programs(0) - 1)
    def _():
        store_grad_rows(acc, (D + FF) // 4, own_ref, xp_ref, send_ref, sem, True)


def mlp_grads(dy, h_t, wo_ref, row_base, zg_ref, zu_ref, dzg_ref, dzu_ref, acc, width, cw, side=None):
    def dz_of(c):
        cols = slice(c * cw, (c + 1) * cw)
        rows = slice(row_base + c * cw, row_base + (c + 1) * cw)
        dm = dot_nt(dy, wo_ref[rows, :]).astype(BF16).astype(F32)
        g = zg_ref[:, cols].astype(F32)
        u = zu_ref[:, cols].astype(F32)
        sig = jax.nn.sigmoid(g)
        sl = g * sig
        du = (dm * sl).astype(BF16)
        dg = (dm * u * (sig + sl * (1.0 - sig))).astype(BF16)
        dzu_ref[:, cols] = du
        dzg_ref[:, cols] = dg
        return dg, du

    def add_dw(c, parts):
        dg, du = parts
        acc[:, c * cw:(c + 1) * cw] += dot(h_t, dg)
        acc[:, width + c * cw:width + (c + 1) * cw] += dot(h_t, du)

    n = width // cw
    prev = dz_of(0)
    for c in range(n):
        nxt = dz_of(c + 1) if c + 1 < n else None
        if side is not None:
            side(c)
        add_dw(c, prev)
        prev = nxt


def bmlp_kernel(half, dy_ref, h_ref, zg_ref, zu_ref, w0, w1, w2, w3, dzg_ref, dzu_ref, own_ref, xp_ref, send_ref,
                wo_ref, acc, sem):
    step = pl.program_id(0)
    hw = FF // 2

    @pl.when(step == 0)
    def _():
        copies = start_rows([((w0, w1, w2, w3), wo_ref)], sem)
        acc[...] = jnp.zeros_like(acc)
        wait_all(copies)

    mlp_grads(dy_ref[...], h_ref[...].T, wo_ref, D + half * hw, zg_ref, zu_ref, dzg_ref, dzu_ref, acc, hw, 256)

    @pl.when(step == pl.num_programs(0) - 1)
    def _():
        store_grad_rows(acc, D // 4, own_ref, xp_ref, send_ref, sem, False)


def bmlp_dwo_kernel(dy_ref, h_ref, o_ref, m_ref, zg_ref, zu_ref, w0, w1, w2, w3, dzg_ref, dzu_ref,
                    oo_ref, ox_ref, os_ref, own_ref, xp_ref, send_ref, wo_ref, acc_o, acc, sem):
    step = pl.program_id(0)

    @pl.when(step == 0)
    def _():
        copies = start_rows([((w0, w1, w2, w3), wo_ref)], sem)
        acc[...] = jnp.zeros_like(acc)
        acc_o[...] = jnp.zeros_like(acc_o)
        wait_all(copies)

    dy = dy_ref[...]
    dy_t = dy.T
    cw = 256

    def side(c):
        acc_o[:, D + c * cw:D + (c + 1) * cw] += dot(dy_t, m_ref[:, c * cw:(c + 1) * cw])

    acc_o[:, 0:D] += dot(dy_t, o_ref[...])
    mlp_grads(dy, h_ref[...].T, wo_ref, D, zg_ref, zu_ref, dzg_ref, dzu_ref, acc, FF, cw, side)

    @pl.when(step == pl.num_programs(0) - 1)
    def _():
        copies = start_grad_rows(acc_o, (D + FF) // 4, oo_ref, ox_ref, os_ref, sem, True)
        copies += start_grad_rows(acc, D // 4, own_ref, xp_ref, send_ref, sem, False, 4)
        wait_all(copies)


def battn_kernel(dy_ref, h_ref, qkv_ref, cs_ref, w0, w1, w2, w3, dz_ref, own_ref, xp_ref, send_ref,
                 wo_ref, acc, c_ref, s_ref, sem):
    step = pl.program_id(0)

    @pl.when(step == 0)
    def _():
        copies = start_rows([((w0, w1, w2, w3), wo_ref)], sem)
        expand_tables(cs_ref, c_ref, s_ref)
        acc[...] = jnp.zeros_like(acc)
        wait_all(copies)

    do_all = dot_nt(dy_ref[...], wo_ref[0:D, :]).astype(BF16)
    lo = lane_iota((SEQ, 2 * HD)) < HD
    tri = tri_mask(128)
    trib = jnp.concatenate([tri] * 2, axis=1)
    for b in range(TOK // SEQ):
        r0 = b * SEQ
        zb = qkv_ref[r0:r0 + SEQ, :]
        do = do_all[r0:r0 + SEQ]
        k0, k1, v0, v1 = kv_tiles(zb[:, D:].astype(F32))
        kt0, kt1 = k0.T.astype(BF16), k1.T.astype(BF16)
        k0, k1, v0, v1 = [t.astype(BF16) for t in (k0, k1, v0, v1)]
        dk = [[None, None], [None, None]]
        dv = [[None, None], [None, None]]
        dq = [[None] * 4, [None] * 4]
        for blk in range(2):
            nk = (blk + 1) * HALF
            rows = slice(blk * HALF, (blk + 1) * HALF)
            k_st = jnp.concatenate([k0[:nk], k1[:nk]], axis=0)
            v_st = jnp.concatenate([v0[:nk], v1[:nk]], axis=0)
            k_t = jnp.concatenate([kt0[:, :nk], kt1[:, :nk]], axis=1)
            dk_b = dv_b = None
            for g in range(2):
                q = jnp.concatenate([zb[rows, (2 * g + i) * 128:(2 * g + i + 1) * 128] for i in range(2)], axis=0)
                dog = jnp.concatenate([do[rows, (2 * g + i) * 128:(2 * g + i + 1) * 128] for i in range(2)], axis=0)
                p = softmax_keys(dot_nt(k_st, q), nk, trib)
                dp = dot_nt(v_st, dog).astype(BF16)
                ds = []
                for i in range(2):
                    dph = [dp[i * nk + k * HALF:i * nk + (k + 1) * HALF].astype(F32) for k in range(nk // HALF)]
                    delta = sum(jnp.sum(a * c, axis=0, keepdims=True) for a, c in zip(dph, p[i]))
                    ds += [(c * (a - delta)).astype(BF16) for a, c in zip(dph, p[i])]
                ds = jnp.concatenate(ds, axis=0)
                pb = jnp.concatenate([t.astype(BF16) for ph in p for t in ph], axis=0)
                dv_g = dot(pb, dog)
                dk_g = dot(ds, q)
                dv_b = dv_g if dv_b is None else dv_b + dv_g
                dk_b = dk_g if dk_b is None else dk_b + dk_g
                dq_t = dot(k_t, ds).T
                for i in range(2):
                    dq[blk][2 * g + i] = dq_t[i * HALF:(i + 1) * HALF]
            for i in range(2):
                for k in range(nk // HALF):
                    sl = slice(i * nk + k * HALF, i * nk + (k + 1) * HALF)
                    dk[i][k] = dk_b[sl] if dk[i][k] is None else dk[i][k] + dk_b[sl]
                    dv[i][k] = dv_b[sl] if dv[i][k] is None else dv[i][k] + dv_b[sl]
        dk0, dk1, dv0, dv1 = [jnp.concatenate(t, axis=0) for t in (dk[0], dk[1], dv[0], dv[1])]
        kpart = dk0 + pltpu.roll(dk1, HD, 1)
        vpart = pltpu.roll(dv0, HD, 1) + dv1
        parts = [jnp.concatenate([dq[0][j], dq[1][j]], axis=0) for j in range(4)]
        parts.append(jnp.where(lo, kpart, vpart))
        for j in range(5):
            tc = slice(0, 128) if j < 4 else slice(128, 256)
            dr = parts[j].astype(BF16).astype(F32)
            dz_ref[r0:r0 + SEQ, j * 128:(j + 1) * 128] = (
                dr * c_ref[:, tc] - half_swap(dr) * s_ref[:, tc]).astype(BF16)
    acc[...] += dot_tn(h_ref[...], dz_ref[...])

    @pl.when(step == pl.num_programs(0) - 1)
    def _():
        store_grad_rows(acc, D // 4, own_ref, xp_ref, send_ref, sem, False)


def dx_kernel(spans, x_ref, gain_ref, dy_ref, dzq_ref, *refs):
    dz_refs = refs[:len(spans)]
    q0, q1, q2, q3, w0, w1, w2, w3, dx_ref, dgain_ref, wq_ref, w_ref, sem = refs[len(spans):]
    step = pl.program_id(0)

    @pl.when(step == 0)
    def _():
        copies = start_rows([((q0, q1, q2, q3), wq_ref), ((w0, w1, w2, w3), w_ref)], sem)
        dgain_ref[...] = jnp.zeros_like(dgain_ref)
        wait_all(copies)

    dh = dot_nt(dzq_ref[...], wq_ref[...])
    for (start, width), dz_ref in zip(spans, dz_refs):
        dh += dot_nt(dz_ref[...], w_ref[:, start:start + width])
    dh = dh.astype(BF16).astype(F32)
    x = x_ref[...].astype(F32)
    cen = x - jnp.mean(x, axis=-1, keepdims=True)
    var = jnp.mean(cen * cen, axis=-1, keepdims=True)
    rstd = lax.rsqrt(var + 1e-6)
    xhat = cen * rstd
    dgain_ref[...] += jnp.sum(dh * xhat, axis=0, keepdims=True)
    dxh = dh * gain_ref[...]
    dx = rstd * (dxh - jnp.mean(dxh, axis=-1, keepdims=True)
                 - xhat * jnp.mean(dxh * xhat, axis=-1, keepdims=True))
    dx_ref[...] = (dy_ref[...].astype(F32) + dx.astype(BF16).astype(F32)).astype(BF16)


ANY = pl.BlockSpec(memory_space=pl.ANY)


def tok_spec(width, block=0, first=0):
    return pl.BlockSpec((TOK, width), lambda i: (i + first, block))


def full_spec(shape):
    return pl.BlockSpec(shape, lambda i: (0,) * len(shape))


def call(kernel, n_tok, in_specs, outs, out_specs, scratch, flops, nbytes, aliases=None):
    return pl.pallas_call(
        kernel,
        grid=(n_tok // TOK,),
        in_specs=in_specs,
        out_specs=out_specs,
        out_shape=[jax.ShapeDtypeStruct(s, t) for s, t in outs],
        scratch_shapes=scratch,
        input_output_aliases=aliases or {},
        compiler_params=pltpu.CompilerParams(
            dimension_semantics=("arbitrary",), vmem_limit_bytes=VMEM_LIMIT),
        cost_estimate=pl.CostEstimate(flops=int(flops), bytes_accessed=int(nbytes), transcendentals=0),
    )


def solution(mesh):
    batch_spec = P(("dp", "fsdp"), None, None)
    scale_spec = P(None, "fsdp")
    weight_spec = P(None, "fsdp", None)

    core_perm = [(0, 1), (1, 0), (2, 3), (3, 2)]
    x_perm = [(0, 2), (2, 0), (1, 3), (3, 1)]
    y_perm = [(0, 1), (1, 0)]

    def pp_core(a):
        return lax.ppermute(a, "fsdp", core_perm)

    def pp_x(a):
        return lax.ppermute(a, "fsdp", x_perm)

    def pp_y(a):
        return lax.ppermute(a, "dp", y_perm)

    def gather4(a):
        far = pp_x(a)
        return (a, pp_core(a), far, pp_core(far))

    def reduce4(own, xp, send):
        recv = pp_core(send)
        far = pp_x(xp + recv[1])
        mine = own + recv[0] + far
        return mine + pp_y(mine)

    def inner_step(x_in, grad_y, norm_scale, w_in, w_out):
        n_layers = w_in.shape[0]
        n_batch = x_in.shape[0]
        n_tok = n_batch * SEQ

        cs_tab = jnp.asarray(rotary_table())

        q_pieces, g_pieces, o_pieces = [], [], []
        for l in range(n_layers):
            wq_l = w_in[l, :, :QKV]
            if l == 0:
                gcols = jnp.pad(norm_scale.T, ((0, 0), (0, 128 - n_layers)))
                wq_l = jnp.concatenate([wq_l, gcols], axis=1)
            q_pieces.append(gather4(wq_l))
            g_pieces.append(gather4(w_in[l, :, QKV:]))
            o_pieces.append(gather4(w_out[l]))
        gp = [a[:, QKV:QKV + n_layers].T for a in q_pieces[0]]
        own = owners()
        slot = jnp.arange(4)[None, :, None]
        gain = sum(jnp.where(slot == own[r], gp[r][:, None, :].astype(F32), 0.0) for r in range(4))
        gain = gain.reshape(n_layers, 1, D)

        x = x_in.reshape(n_tok, D)
        mm = 2.0 * n_tok * D
        saved = []
        sem = pltpu.SemaphoreType.DMA
        for l in range(n_layers):
            h, qkv, o = call(
                fwd_attn_kernel, n_tok,
                [tok_spec(D), full_spec((1, D)), full_spec((SEQ, 128))] + [ANY] * 4,
                [((n_tok, D), BF16), ((n_tok, QKV), BF16), ((n_tok, D), BF16)],
                [tok_spec(D), tok_spec(QKV), tok_spec(D)],
                [pltpu.VMEM((D, QKV), BF16), pltpu.VMEM((SEQ, 256), F32), pltpu.VMEM((SEQ, 256), F32), sem((4,))],
                mm * 2600, n_tok * D * 8,
            )(x, gain[l], cs_tab, *q_pieces[l])
            z, m, y = call(
                fwd_mlp_kernel, n_tok,
                [tok_spec(D), tok_spec(D), tok_spec(D)] + [ANY] * 8,
                [((n_tok, 2 * FF), BF16), ((n_tok, FF), BF16), ((n_tok, D), BF16)],
                [tok_spec(2 * FF), tok_spec(FF), tok_spec(D)],
                [pltpu.VMEM((D, 2 * FF), BF16), pltpu.VMEM((D + FF, D), BF16), sem((8,))],
                mm * 6700, n_tok * D * 32,
            )(x, h, o, *g_pieces[l], *o_pieces[l])
            saved.append((x, h, qkv, o, z, m))
            x = y

        dy = grad_y.reshape(n_tok, D)
        d_gain = [None] * n_layers
        d_win = [None] * n_layers
        d_wout = [None] * n_layers
        q4 = (D + FF) // 4

        def grad_outs(shape):
            return [(shape, F32), (shape, F32), ((2,) + shape, F32)]

        for l in reversed(range(n_layers)):
            xl, h, qkv, o, z, m = saved[l]
            hw = FF // 2
            n_half = 2 if l == 0 else 1
            fw = FF // n_half
            dzs, spans, win_parts = [], [], []
            if n_half == 1:
                dg, du, *g = call(
                    bmlp_dwo_kernel, n_tok,
                    [tok_spec(D)] * 3 + [tok_spec(FF), tok_spec(FF, 0), tok_spec(FF, 1)] + [ANY] * 4,
                    [((n_tok, FF), BF16), ((n_tok, FF), BF16)] + grad_outs((D, q4)) + grad_outs((D // 4, 2 * FF)),
                    [tok_spec(FF), tok_spec(FF)] + [ANY] * 6,
                    [pltpu.VMEM((D + FF, D), BF16), pltpu.VMEM((D, D + FF), F32), pltpu.VMEM((D, 2 * FF), F32),
                     sem((8,))],
                    mm * 8704, n_tok * D * 50,
                )(dy, h, o, m, z, z, *o_pieces[l])
                dzs, spans = [dg, du], [(0, FF), (FF, FF)]
                d_wout[l] = reduce4(*g[:3]).T
                win_parts.append(reduce4(*g[3:]))
            else:
                g = call(
                    dwo_kernel, n_tok, [tok_spec(D), tok_spec(D), tok_spec(FF)],
                    grad_outs((D, q4)), [ANY] * 3,
                    [pltpu.VMEM((D, D + FF), F32), sem((4,))],
                    mm * 2560, n_tok * D * 12,
                )(dy, o, m)
                d_wout[l] = reduce4(*g).T
                for hf in range(2):
                    dg, du, *g = call(
                        functools.partial(bmlp_kernel, hf), n_tok,
                        [tok_spec(D), tok_spec(D), tok_spec(hw, hf), tok_spec(hw, 2 + hf)] + [ANY] * 4,
                        [((n_tok, hw), BF16), ((n_tok, hw), BF16)] + grad_outs((D // 4, 2 * hw)),
                        [tok_spec(hw), tok_spec(hw)] + [ANY] * 3,
                        [pltpu.VMEM((D + FF, D), BF16), pltpu.VMEM((D, 2 * hw), F32), sem((4,))],
                        mm * 3072, n_tok * D * 20,
                    )(dy, h, z, z, *o_pieces[l])
                    dzs += [dg, du]
                    spans += [(hf * hw, hw), (FF + hf * hw, hw)]
                    win_parts.append(reduce4(*g))
            dzq, *g = call(
                battn_kernel, n_tok,
                [tok_spec(D), tok_spec(D), tok_spec(QKV), full_spec((SEQ, 128))] + [ANY] * 4,
                [((n_tok, QKV), BF16)] + grad_outs((D // 4, QKV)),
                [tok_spec(QKV)] + [ANY] * 3,
                [pltpu.VMEM((D + FF, D), BF16), pltpu.VMEM((D, QKV), F32), pltpu.VMEM((SEQ, 256), F32),
                 pltpu.VMEM((SEQ, 256), F32), sem((4,))],
                mm * 6200, n_tok * D * 10,
            )(dy, h, qkv, cs_tab, *o_pieces[l])
            wq = reduce4(*g)
            d_win[l] = jnp.concatenate(
                [wq] + [p[:, :fw] for p in win_parts] + [p[:, fw:] for p in win_parts], axis=1)
            dy, d_gain[l] = call(
                functools.partial(dx_kernel, tuple(spans)), n_tok,
                [tok_spec(D), full_spec((1, D)), tok_spec(D), tok_spec(QKV)] + [tok_spec(fw)] * len(dzs) + [ANY] * 8,
                [((n_tok, D), BF16), ((1, D), F32)],
                [tok_spec(D), full_spec((1, D))],
                [pltpu.VMEM((D, QKV), BF16), pltpu.VMEM((D, 2 * FF), BF16), sem((8,))],
                mm * 4736, n_tok * D * 20,
            )(xl, gain[l], dy, dzq, *dzs, *q_pieces[l], *g_pieces[l])

        gg = jnp.concatenate(d_gain, axis=0)
        gg = gg + pp_core(gg)
        gg = gg + pp_x(gg)
        gg, g_wout = lax.optimization_barrier((gg, jnp.stack(d_wout)))
        gg = gg + pp_y(gg)
        gg = lax.dynamic_slice(gg, (0, lax.axis_index("fsdp") * (D // 4)), (n_layers, D // 4))
        return (x.reshape(x_in.shape), dy.reshape(x_in.shape), gg, jnp.stack(d_win), g_wout)

    return jax.shard_map(
        inner_step,
        mesh=mesh,
        in_specs=(batch_spec, batch_spec, scale_spec, weight_spec, weight_spec),
        out_specs=(batch_spec, batch_spec, scale_spec, weight_spec, weight_spec),
        check_vma=False,
    )
```

```python
import functools
import jax
import numpy as np
import jax.numpy as jnp
from jax import lax
from jax.experimental import pallas as pl
from jax.experimental.pallas import tpu as pltpu
from jax.sharding import PartitionSpec as P

F32 = jnp.float32
BF16 = jnp.bfloat16
SEQ = 256
HD = 64
D = 512
FF = 2048
QKV = D + 2 * HD
NEG = -1e30
VMEM_LIMIT = 60 * 1024 * 1024

TOK = 512


def dot(a, b):
    return jnp.dot(a, b, preferred_element_type=F32)


def dot_nt(a, b):
    return lax.dot_general(a, b, (((1,), (1,)), ((), ())), preferred_element_type=F32)


def dot_tn(a, b):
    return lax.dot_general(a, b, (((0,), (0,)), ((), ())), preferred_element_type=F32)


def owners():
    me = lax.axis_index("fsdp")
    x = me // 2
    c = me - 2 * x
    return [2 * x + c, 2 * x + (1 - c), 2 * (1 - x) + c, 2 * (1 - x) + (1 - c)]


def start_rows(groups, sem):
    own = owners()
    copies = []
    for pieces, dst in groups:
        rows = pieces[0].shape[0]
        for r in range(4):
            start = pl.multiple_of(own[r] * rows, rows)
            src = pieces[r].at[:, pl.ds(0, dst.shape[1])]
            cp = pltpu.make_async_copy(src, dst.at[pl.ds(start, rows), :], sem.at[len(copies)])
            cp.start()
            copies.append(cp)
    return copies


def wait_all(copies):
    for cp in copies:
        cp.wait()


def lane_iota(shape):
    return lax.broadcasted_iota(jnp.int32, shape, len(shape) - 1)


def half_swap(z):
    n = z.shape[-1]
    lo = lax.rem(lane_iota(z.shape), HD) < HD // 2
    return jnp.where(lo, pltpu.roll(z, n - HD // 2, 1), pltpu.roll(z, HD // 2, 1))


HALF = SEQ // 2


def kv_tiles(kv):
    lo = lane_iota(kv.shape) < HD
    rolled = pltpu.roll(kv, HD, 1)
    zero = jnp.zeros_like(kv)
    return (jnp.where(lo, kv, zero), jnp.where(lo, zero, rolled),
            jnp.where(lo, rolled, zero), jnp.where(lo, zero, kv))


def tri_mask(n):
    key = lax.broadcasted_iota(jnp.int32, (HALF, n), 0)
    query = lax.rem(lax.broadcasted_iota(jnp.int32, (HALF, n), 1), HALF)
    return query >= key


def softmax_keys(s, n_keys, tri):
    out = []
    for i in range(2):
        sh = s[i * n_keys:(i + 1) * n_keys]
        sh = [sh[k * HALF:(k + 1) * HALF] for k in range(n_keys // HALF)]
        sh[-1] = jnp.where(tri, sh[-1], NEG)
        m = jnp.max(sh[-1], axis=0, keepdims=True)
        for t in sh[:-1]:
            m = jnp.maximum(m, jnp.max(t, axis=0, keepdims=True))
        e = [jnp.exp(t - m) for t in sh]
        l = jnp.sum(e[0], axis=0, keepdims=True)
        for t in e[1:]:
            l = l + jnp.sum(t, axis=0, keepdims=True)
        inv = 1.0 / l
        out.append([t * inv for t in e])
    return out


def expand_tables(cs_ref, c_ref, s_ref):
    cs = cs_ref[...]
    lo = lane_iota(cs.shape) < HD
    rolled = pltpu.roll(cs, HD, 1)
    cos = jnp.where(lo, cs, rolled)
    sin = jnp.where(lo, rolled, cs)
    c_ref[:, 0:128] = cos * HD ** -0.5
    s_ref[:, 0:128] = sin * HD ** -0.5
    c_ref[:, 128:256] = jnp.where(lo, cos, 1.0)
    s_ref[:, 128:256] = jnp.where(lo, sin, 0.0)


def rotary_table():
    half = HD // 2
    inv_freq = np.float32(10000.0) ** (-(np.arange(half, dtype=np.float32) * np.float32(2.0 / HD)))
    angles = np.arange(SEQ, dtype=np.float32)[:, None] * inv_freq[None, :]
    cos, sin = np.cos(angles), np.sin(angles)
    return np.concatenate([cos, cos, -sin, sin], axis=1).astype(np.float32)


def fwd_attn_kernel(x_ref, gain_ref, cs_ref, w0, w1, w2, w3, h_ref, qkv_ref, o_ref, w_ref, c_ref, s_ref, sem):
    @pl.when(pl.program_id(0) == 0)
    def _():
        copies = start_rows([((w0, w1, w2, w3), w_ref)], sem)
        expand_tables(cs_ref, c_ref, s_ref)
        wait_all(copies)

    x = x_ref[...].astype(F32)
    cen = x - jnp.mean(x, axis=-1, keepdims=True)
    var = jnp.mean(cen * cen, axis=-1, keepdims=True)
    h = (cen * lax.rsqrt(var + 1e-6) * gain_ref[...]).astype(BF16)
    h_ref[...] = h
    z_all = dot(h, w_ref[...]).astype(BF16)
    tri = tri_mask(128)
    for b in range(TOK // SEQ):
        r0 = b * SEQ
        zt = []
        for j in range(5):
            t = z_all[r0:r0 + SEQ, j * 128:(j + 1) * 128].astype(F32)
            tc = slice(0, 128) if j < 4 else slice(128, 256)
            t = (t * c_ref[:, tc] + half_swap(t) * s_ref[:, tc]).astype(BF16)
            qkv_ref[r0:r0 + SEQ, j * 128:(j + 1) * 128] = t
            zt.append(t)
        k0, k1, v0, v1 = kv_tiles(zt[4].astype(F32))
        k0, k1 = k0.astype(BF16), k1.astype(BF16)
        v0, v1 = v0.T.astype(BF16), v1.T.astype(BF16)
        for blk in range(2):
            nk = (blk + 1) * HALF
            rows = slice(blk * HALF, (blk + 1) * HALF)
            k_st = jnp.concatenate([k0[:nk], k1[:nk]], axis=0)
            v_t = jnp.concatenate([v0[:, :nk], v1[:, :nk]], axis=1)
            for g in range(2):
                q = jnp.concatenate([zt[2 * g + i][rows] for i in range(2)], axis=0)
                s = dot_nt(k_st, q)
                trib = jnp.concatenate([tri] * 2, axis=1)
                p = softmax_keys(s, nk, trib)
                pb = jnp.concatenate([t.astype(BF16) for ph in p for t in ph], axis=0)
                o = dot(v_t, pb).T.astype(BF16)
                for i in range(2):
                    j = 2 * g + i
                    o_ref[r0 + blk * HALF:r0 + (blk + 1) * HALF, j * 128:(j + 1) * 128] = o[i * HALF:(i + 1) * HALF]


def fwd_mlp_kernel(x_ref, h_ref, o_ref, g0, g1, g2, g3, u0, u1, u2, u3, z_ref, m_ref, y_ref, w_ref, wo_ref, sem):
    @pl.when(pl.program_id(0) == 0)
    def _():
        copies = start_rows([((g0, g1, g2, g3), w_ref), ((u0, u1, u2, u3), wo_ref)], sem)
        wait_all(copies)

    h = h_ref[...]
    cw = 512
    acc = dot(o_ref[...], wo_ref[0:D, :])
    for c in range(FF // cw):
        gc = slice(c * cw, (c + 1) * cw)
        uc = slice(FF + c * cw, FF + (c + 1) * cw)
        g = dot(h, w_ref[:, gc]).astype(BF16)
        u = dot(h, w_ref[:, uc]).astype(BF16)
        z_ref[:, gc] = g
        z_ref[:, uc] = u
        g = g.astype(F32)
        m = (g * jax.nn.sigmoid(g) * u.astype(F32)).astype(BF16)
        m_ref[:, gc] = m
        acc = acc + dot(m, wo_ref[D + c * cw:D + (c + 1) * cw, :])
    y_ref[...] = (x_ref[...].astype(F32) + acc).astype(BF16)


def start_grad_rows(acc, width, own_ref, xp_ref, send_ref, sem, by_cols, first=0):
    own = owners()
    copies = []
    for r, dst in ((1, send_ref.at[0]), (3, send_ref.at[1]), (0, own_ref), (2, xp_ref)):
        start = pl.multiple_of(own[r] * width, 128)
        src = acc.at[:, pl.ds(start, width)] if by_cols else acc.at[pl.ds(start, width), :]
        cp = pltpu.make_async_copy(src, dst, sem.at[first + r])
        cp.start()
        copies.append(cp)
    return copies


def store_grad_rows(*args):
    wait_all(start_grad_rows(*args))


def dwo_kernel(dy_ref, o_ref, m_ref, own_ref, xp_ref, send_ref, acc, sem):
    step = pl.program_id(0)

    @pl.when(step == 0)
    def _():
        acc[...] = jnp.zeros_like(acc)

    dy = dy_ref[...]
    acc[:, 0:D] += dot_tn(dy, o_ref[...])
    cw = 512
    for c in range(FF // cw):
        acc[:, D + c * cw:D + (c + 1) * cw] += dot_tn(dy, m_ref[:, c * cw:(c + 1) * cw])

    @pl.when(step == pl.num_programs(0) - 1)
    def _():
        store_grad_rows(acc, (D + FF) // 4, own_ref, xp_ref, send_ref, sem, True)


def mlp_grads(dy, h_t, wo_ref, row_base, zg_ref, zu_ref, dzg_ref, dzu_ref, acc, width, cw, side=None):
    def dz_of(c):
        cols = slice(c * cw, (c + 1) * cw)
        rows = slice(row_base + c * cw, row_base + (c + 1) * cw)
        dm = dot_nt(dy, wo_ref[rows, :]).astype(BF16).astype(F32)
        g = zg_ref[:, cols].astype(F32)
        u = zu_ref[:, cols].astype(F32)
        sig = jax.nn.sigmoid(g)
        sl = g * sig
        du = (dm * sl).astype(BF16)
        dg = (dm * u * (sig + sl * (1.0 - sig))).astype(BF16)
        dzu_ref[:, cols] = du
        dzg_ref[:, cols] = dg
        return dg, du

    def add_dw(c, parts):
        dg, du = parts
        acc[:, c * cw:(c + 1) * cw] += dot(h_t, dg)
        acc[:, width + c * cw:width + (c + 1) * cw] += dot(h_t, du)

    n = width // cw
    prev = dz_of(0)
    for c in range(n):
        nxt = dz_of(c + 1) if c + 1 < n else None
        if side is not None:
            side(c)
        add_dw(c, prev)
        prev = nxt


def bmlp_kernel(half, dy_ref, h_ref, zg_ref, zu_ref, w0, w1, w2, w3, dzg_ref, dzu_ref, own_ref, xp_ref, send_ref,
                wo_ref, acc, sem):
    step = pl.program_id(0)
    hw = FF // 2

    @pl.when(step == 0)
    def _():
        copies = start_rows([((w0, w1, w2, w3), wo_ref)], sem)
        acc[...] = jnp.zeros_like(acc)
        wait_all(copies)

    mlp_grads(dy_ref[...], h_ref[...].T, wo_ref, D + half * hw, zg_ref, zu_ref, dzg_ref, dzu_ref, acc, hw, 256)

    @pl.when(step == pl.num_programs(0) - 1)
    def _():
        store_grad_rows(acc, D // 4, own_ref, xp_ref, send_ref, sem, False)


def bmlp_dwo_kernel(dy_ref, h_ref, o_ref, m_ref, zg_ref, zu_ref, w0, w1, w2, w3, dzg_ref, dzu_ref,
                    oo_ref, ox_ref, os_ref, own_ref, xp_ref, send_ref, wo_ref, acc_o, acc, sem):
    step = pl.program_id(0)

    @pl.when(step == 0)
    def _():
        copies = start_rows([((w0, w1, w2, w3), wo_ref)], sem)
        acc[...] = jnp.zeros_like(acc)
        acc_o[...] = jnp.zeros_like(acc_o)
        wait_all(copies)

    dy = dy_ref[...]
    dy_t = dy.T
    cw = 256

    def side(c):
        acc_o[:, D + c * cw:D + (c + 1) * cw] += dot(dy_t, m_ref[:, c * cw:(c + 1) * cw])

    acc_o[:, 0:D] += dot(dy_t, o_ref[...])
    mlp_grads(dy, h_ref[...].T, wo_ref, D, zg_ref, zu_ref, dzg_ref, dzu_ref, acc, FF, cw, side)

    @pl.when(step == pl.num_programs(0) - 1)
    def _():
        copies = start_grad_rows(acc_o, (D + FF) // 4, oo_ref, ox_ref, os_ref, sem, True)
        copies += start_grad_rows(acc, D // 4, own_ref, xp_ref, send_ref, sem, False, 4)
        wait_all(copies)


def battn_kernel(dy_ref, h_ref, qkv_ref, cs_ref, w0, w1, w2, w3, dz_ref, own_ref, xp_ref, send_ref,
                 wo_ref, acc, c_ref, s_ref, sem):
    step = pl.program_id(0)

    @pl.when(step == 0)
    def _():
        copies = start_rows([((w0, w1, w2, w3), wo_ref)], sem)
        expand_tables(cs_ref, c_ref, s_ref)
        acc[...] = jnp.zeros_like(acc)
        wait_all(copies)

    do_all = dot_nt(dy_ref[...], wo_ref[0:D, :]).astype(BF16)
    lo = lane_iota((SEQ, 2 * HD)) < HD
    tri = tri_mask(128)
    trib = jnp.concatenate([tri] * 2, axis=1)
    for b in range(TOK // SEQ):
        r0 = b * SEQ
        zb = qkv_ref[r0:r0 + SEQ, :]
        do = do_all[r0:r0 + SEQ]
        k0, k1, v0, v1 = kv_tiles(zb[:, D:].astype(F32))
        kt0, kt1 = k0.T.astype(BF16), k1.T.astype(BF16)
        k0, k1, v0, v1 = [t.astype(BF16) for t in (k0, k1, v0, v1)]
        dk = [[None, None], [None, None]]
        dv = [[None, None], [None, None]]
        dq = [[None] * 4, [None] * 4]
        for blk in range(2):
            nk = (blk + 1) * HALF
            rows = slice(blk * HALF, (blk + 1) * HALF)
            k_st = jnp.concatenate([k0[:nk], k1[:nk]], axis=0)
            v_st = jnp.concatenate([v0[:nk], v1[:nk]], axis=0)
            k_t = jnp.concatenate([kt0[:, :nk], kt1[:, :nk]], axis=1)
            dk_b = dv_b = None
            for g in range(2):
                q = jnp.concatenate([zb[rows, (2 * g + i) * 128:(2 * g + i + 1) * 128] for i in range(2)], axis=0)
                dog = jnp.concatenate([do[rows, (2 * g + i) * 128:(2 * g + i + 1) * 128] for i in range(2)], axis=0)
                p = softmax_keys(dot_nt(k_st, q), nk, trib)
                dp = dot_nt(v_st, dog).astype(BF16)
                ds = []
                for i in range(2):
                    dph = [dp[i * nk + k * HALF:i * nk + (k + 1) * HALF].astype(F32) for k in range(nk // HALF)]
                    delta = sum(jnp.sum(a * c, axis=0, keepdims=True) for a, c in zip(dph, p[i]))
                    ds += [(c * (a - delta)).astype(BF16) for a, c in zip(dph, p[i])]
                ds = jnp.concatenate(ds, axis=0)
                pb = jnp.concatenate([t.astype(BF16) for ph in p for t in ph], axis=0)
                dv_g = dot(pb, dog)
                dk_g = dot(ds, q)
                dv_b = dv_g if dv_b is None else dv_b + dv_g
                dk_b = dk_g if dk_b is None else dk_b + dk_g
                dq_t = dot(k_t, ds).T
                for i in range(2):
                    dq[blk][2 * g + i] = dq_t[i * HALF:(i + 1) * HALF]
            for i in range(2):
                for k in range(nk // HALF):
                    sl = slice(i * nk + k * HALF, i * nk + (k + 1) * HALF)
                    dk[i][k] = dk_b[sl] if dk[i][k] is None else dk[i][k] + dk_b[sl]
                    dv[i][k] = dv_b[sl] if dv[i][k] is None else dv[i][k] + dv_b[sl]
        dk0, dk1, dv0, dv1 = [jnp.concatenate(t, axis=0) for t in (dk[0], dk[1], dv[0], dv[1])]
        kpart = dk0 + pltpu.roll(dk1, HD, 1)
        vpart = pltpu.roll(dv0, HD, 1) + dv1
        parts = [jnp.concatenate([dq[0][j], dq[1][j]], axis=0) for j in range(4)]
        parts.append(jnp.where(lo, kpart, vpart))
        for j in range(5):
            tc = slice(0, 128) if j < 4 else slice(128, 256)
            dr = parts[j].astype(BF16).astype(F32)
            dz_ref[r0:r0 + SEQ, j * 128:(j + 1) * 128] = (
                dr * c_ref[:, tc] - half_swap(dr) * s_ref[:, tc]).astype(BF16)
    acc[...] += dot_tn(h_ref[...], dz_ref[...])

    @pl.when(step == pl.num_programs(0) - 1)
    def _():
        store_grad_rows(acc, D // 4, own_ref, xp_ref, send_ref, sem, False)


def dx_kernel(spans, x_ref, gain_ref, dy_ref, dzq_ref, *refs):
    dz_refs = refs[:len(spans)]
    q0, q1, q2, q3, w0, w1, w2, w3, dx_ref, dgain_ref, wq_ref, w_ref, sem = refs[len(spans):]
    step = pl.program_id(0)

    @pl.when(step == 0)
    def _():
        copies = start_rows([((q0, q1, q2, q3), wq_ref), ((w0, w1, w2, w3), w_ref)], sem)
        dgain_ref[...] = jnp.zeros_like(dgain_ref)
        wait_all(copies)

    dh = dot_nt(dzq_ref[...], wq_ref[...])
    for (start, width), dz_ref in zip(spans, dz_refs):
        dh += dot_nt(dz_ref[...], w_ref[:, start:start + width])
    dh = dh.astype(BF16).astype(F32)
    x = x_ref[...].astype(F32)
    cen = x - jnp.mean(x, axis=-1, keepdims=True)
    var = jnp.mean(cen * cen, axis=-1, keepdims=True)
    rstd = lax.rsqrt(var + 1e-6)
    xhat = cen * rstd
    dgain_ref[...] += jnp.sum(dh * xhat, axis=0, keepdims=True)
    dxh = dh * gain_ref[...]
    dx = rstd * (dxh - jnp.mean(dxh, axis=-1, keepdims=True)
                 - xhat * jnp.mean(dxh * xhat, axis=-1, keepdims=True))
    dx_ref[...] = (dy_ref[...].astype(F32) + dx.astype(BF16).astype(F32)).astype(BF16)


def place_win_kernel(moves, *refs):
    out_ref = refs[-1]
    for k, group in enumerate(moves):
        a_ref, b_ref = refs[2 * k], refs[2 * k + 1]
        for src, dst, width in group:
            out_ref[0, :, dst:dst + width] = a_ref[:, src:src + width] + b_ref[:, src:src + width]


def place_wout_kernel(a_ref, b_ref, *rest):
    out_ref = rest[-1]
    out_ref[0] = (a_ref[...] + b_ref[...]).T


ANY = pl.BlockSpec(memory_space=pl.ANY)


def tok_spec(width, block=0, first=0):
    return pl.BlockSpec((TOK, width), lambda i: (i + first, block))


def full_spec(shape):
    return pl.BlockSpec(shape, lambda i: (0,) * len(shape))


def call(kernel, n_tok, in_specs, outs, out_specs, scratch, flops, nbytes, aliases=None):
    return pl.pallas_call(
        kernel,
        grid=(n_tok // TOK,),
        in_specs=in_specs,
        out_specs=out_specs,
        out_shape=[jax.ShapeDtypeStruct(s, t) for s, t in outs],
        scratch_shapes=scratch,
        input_output_aliases=aliases or {},
        compiler_params=pltpu.CompilerParams(
            dimension_semantics=("arbitrary",), vmem_limit_bytes=VMEM_LIMIT),
        cost_estimate=pl.CostEstimate(flops=int(flops), bytes_accessed=int(nbytes), transcendentals=0),
    )


def solution(mesh):
    batch_spec = P(("dp", "fsdp"), None, None)
    scale_spec = P(None, "fsdp")
    weight_spec = P(None, "fsdp", None)

    core_perm = [(0, 1), (1, 0), (2, 3), (3, 2)]
    x_perm = [(0, 2), (2, 0), (1, 3), (3, 1)]
    y_perm = [(0, 1), (1, 0)]

    def pp_core(a):
        return lax.ppermute(a, "fsdp", core_perm)

    def pp_x(a):
        return lax.ppermute(a, "fsdp", x_perm)

    def pp_y(a):
        return lax.ppermute(a, "dp", y_perm)

    def gather4(a):
        far = pp_x(a)
        return (a, pp_core(a), far, pp_core(far))

    def reduce4(own, xp, send):
        recv = pp_core(send)
        far = pp_x(xp + recv[1])
        mine = own + recv[0] + far
        return mine, pp_y(mine)

    def inner_step(x_in, grad_y, norm_scale, w_in, w_out):
        n_layers = w_in.shape[0]
        n_batch = x_in.shape[0]
        n_tok = n_batch * SEQ

        cs_tab = jnp.asarray(rotary_table())

        q_pieces, g_pieces, o_pieces = [], [], []
        for l in range(n_layers):
            wq_l = w_in[l, :, :QKV]
            if l == 0:
                gcols = jnp.pad(norm_scale.T, ((0, 0), (0, 128 - n_layers)))
                wq_l = jnp.concatenate([wq_l, gcols], axis=1)
            q_pieces.append(gather4(wq_l))
            g_pieces.append(gather4(w_in[l, :, QKV:]))
            o_pieces.append(gather4(w_out[l]))
        gp = [a[:, QKV:QKV + n_layers].T for a in q_pieces[0]]
        own = owners()
        slot = jnp.arange(4)[None, :, None]
        gain = sum(jnp.where(slot == own[r], gp[r][:, None, :].astype(F32), 0.0) for r in range(4))
        gain = gain.reshape(n_layers, 1, D)

        x = x_in.reshape(n_tok, D)
        mm = 2.0 * n_tok * D
        saved = []
        sem = pltpu.SemaphoreType.DMA
        for l in range(n_layers):
            h, qkv, o = call(
                fwd_attn_kernel, n_tok,
                [tok_spec(D), full_spec((1, D)), full_spec((SEQ, 128))] + [ANY] * 4,
                [((n_tok, D), BF16), ((n_tok, QKV), BF16), ((n_tok, D), BF16)],
                [tok_spec(D), tok_spec(QKV), tok_spec(D)],
                [pltpu.VMEM((D, QKV), BF16), pltpu.VMEM((SEQ, 256), F32), pltpu.VMEM((SEQ, 256), F32), sem((4,))],
                mm * 2600, n_tok * D * 8,
            )(x, gain[l], cs_tab, *q_pieces[l])
            z, m, y = call(
                fwd_mlp_kernel, n_tok,
                [tok_spec(D), tok_spec(D), tok_spec(D)] + [ANY] * 8,
                [((n_tok, 2 * FF), BF16), ((n_tok, FF), BF16), ((n_tok, D), BF16)],
                [tok_spec(2 * FF), tok_spec(FF), tok_spec(D)],
                [pltpu.VMEM((D, 2 * FF), BF16), pltpu.VMEM((D + FF, D), BF16), sem((8,))],
                mm * 6700, n_tok * D * 32,
            )(x, h, o, *g_pieces[l], *o_pieces[l])
            saved.append((x, h, qkv, o, z, m))
            x = y

        dy = grad_y.reshape(n_tok, D)
        d_gain = [None] * n_layers
        d_win = [None] * n_layers
        d_wout = [None] * n_layers
        q4 = (D + FF) // 4

        def grad_outs(shape):
            return [(shape, F32), (shape, F32), ((2,) + shape, F32)]

        for l in reversed(range(n_layers)):
            xl, h, qkv, o, z, m = saved[l]
            hw = FF // 2
            n_half = 2 if l == 0 else 1
            fw = FF // n_half
            dzs, spans, win_parts = [], [], []
            if n_half == 1:
                dg, du, *g = call(
                    bmlp_dwo_kernel, n_tok,
                    [tok_spec(D)] * 3 + [tok_spec(FF), tok_spec(FF, 0), tok_spec(FF, 1)] + [ANY] * 4,
                    [((n_tok, FF), BF16), ((n_tok, FF), BF16)] + grad_outs((D, q4)) + grad_outs((D // 4, 2 * FF)),
                    [tok_spec(FF), tok_spec(FF)] + [ANY] * 6,
                    [pltpu.VMEM((D + FF, D), BF16), pltpu.VMEM((D, D + FF), F32), pltpu.VMEM((D, 2 * FF), F32),
                     sem((8,))],
                    mm * 8704, n_tok * D * 50,
                )(dy, h, o, m, z, z, *o_pieces[l])
                dzs, spans = [dg, du], [(0, FF), (FF, FF)]
                d_wout[l] = reduce4(*g[:3])
                win_parts.append(reduce4(*g[3:]))
            else:
                g = call(
                    dwo_kernel, n_tok, [tok_spec(D), tok_spec(D), tok_spec(FF)],
                    grad_outs((D, q4)), [ANY] * 3,
                    [pltpu.VMEM((D, D + FF), F32), sem((4,))],
                    mm * 2560, n_tok * D * 12,
                )(dy, o, m)
                d_wout[l] = reduce4(*g)
                for hf in range(2):
                    dg, du, *g = call(
                        functools.partial(bmlp_kernel, hf), n_tok,
                        [tok_spec(D), tok_spec(D), tok_spec(hw, hf), tok_spec(hw, 2 + hf)] + [ANY] * 4,
                        [((n_tok, hw), BF16), ((n_tok, hw), BF16)] + grad_outs((D // 4, 2 * hw)),
                        [tok_spec(hw), tok_spec(hw)] + [ANY] * 3,
                        [pltpu.VMEM((D + FF, D), BF16), pltpu.VMEM((D, 2 * hw), F32), sem((4,))],
                        mm * 3072, n_tok * D * 20,
                    )(dy, h, z, z, *o_pieces[l])
                    dzs += [dg, du]
                    spans += [(hf * hw, hw), (FF + hf * hw, hw)]
                    win_parts.append(reduce4(*g))
            dzq, *g = call(
                battn_kernel, n_tok,
                [tok_spec(D), tok_spec(D), tok_spec(QKV), full_spec((SEQ, 128))] + [ANY] * 4,
                [((n_tok, QKV), BF16)] + grad_outs((D // 4, QKV)),
                [tok_spec(QKV)] + [ANY] * 3,
                [pltpu.VMEM((D + FF, D), BF16), pltpu.VMEM((D, QKV), F32), pltpu.VMEM((SEQ, 256), F32),
                 pltpu.VMEM((SEQ, 256), F32), sem((4,))],
                mm * 6200, n_tok * D * 10,
            )(dy, h, qkv, cs_tab, *o_pieces[l])
            wq = reduce4(*g)
            d_win[l] = [(wq, ((0, 0, QKV),))] + [
                (p, ((0, QKV + i * fw, fw), (fw, QKV + FF + i * fw, fw))) for i, p in enumerate(win_parts)]
            dy, d_gain[l] = call(
                functools.partial(dx_kernel, tuple(spans)), n_tok,
                [tok_spec(D), full_spec((1, D)), tok_spec(D), tok_spec(QKV)] + [tok_spec(fw)] * len(dzs) + [ANY] * 8,
                [((n_tok, D), BF16), ((1, D), F32)],
                [tok_spec(D), full_spec((1, D))],
                [pltpu.VMEM((D, QKV), BF16), pltpu.VMEM((D, 2 * FF), BF16), sem((8,))],
                mm * 4736, n_tok * D * 20,
            )(xl, gain[l], dy, dzq, *dzs, *q_pieces[l], *g_pieces[l])

        g_win, g_wout = None, None
        rows = D // 4
        for l in reversed(range(n_layers)):
            layer_row = functools.partial(lambda layer, i: (layer, i, 0), l)
            prev = () if g_win is None else (g_win,)
            args = [a for pair, _ in d_win[l] for a in pair]
            g_win = pl.pallas_call(
                functools.partial(place_win_kernel, tuple(m for _, m in d_win[l])),
                grid=(8,),
                in_specs=[pl.BlockSpec((rows // 8, a.shape[1]), lambda i: (i, 0)) for a in args] + [ANY] * len(prev),
                out_specs=pl.BlockSpec((1, rows // 8, QKV + 2 * FF), layer_row),
                out_shape=jax.ShapeDtypeStruct((n_layers, rows, QKV + 2 * FF), F32),
                input_output_aliases={len(args): 0} if prev else {},
                cost_estimate=pl.CostEstimate(flops=10 ** 6, bytes_accessed=10 ** 7, transcendentals=0),
            )(*args, *prev)
            prev = () if g_wout is None else (g_wout,)
            g_wout = pl.pallas_call(
                place_wout_kernel,
                grid=(q4 // 128,),
                in_specs=[pl.BlockSpec((D, 128), lambda i: (0, i))] * 2 + [ANY] * len(prev),
                out_specs=pl.BlockSpec((1, 128, D), layer_row),
                out_shape=jax.ShapeDtypeStruct((n_layers, q4, D), F32),
                input_output_aliases={2: 0} if prev else {},
                cost_estimate=pl.CostEstimate(flops=10 ** 6, bytes_accessed=4 * 10 ** 6, transcendentals=0),
            )(*d_wout[l], *prev)

        gg = jnp.concatenate(d_gain, axis=0)
        gg = gg + pp_core(gg)
        gg = gg + pp_x(gg)
        gg, g_wout = lax.optimization_barrier((gg, g_wout))
        gg = gg + pp_y(gg)
        gg = lax.dynamic_slice(gg, (0, lax.axis_index("fsdp") * (D // 4)), (n_layers, D // 4))
        return (x.reshape(x_in.shape), dy.reshape(x_in.shape), gg, g_win, g_wout)

    return jax.shard_map(
        inner_step,
        mesh=mesh,
        in_specs=(batch_spec, batch_spec, scale_spec, weight_spec, weight_spec),
        out_specs=(batch_spec, batch_spec, scale_spec, weight_spec, weight_spec),
        check_vma=False,
    )
```
